128 devices in a mesh: dp: 1, tp: 2 (over core), sp: 64 (over z, y, x).
Axes of the slice: x: 4, y: 4, z: 4, core: 2. Of those that a mesh axis runs over, the one named last changes fastest.
Arguments:
- hidden: bfloat16 [4, 8192], P('dp')
- norm_gain: float32 [8192], replicated
- w_query: bfloat16 [8192, 8192], P(None, 'tp')
- w_key: bfloat16 [8192, 1024], P(None, 'tp')
- w_value: bfloat16 [8192, 1024], P(None, 'tp')
- w_out: bfloat16 [8192, 8192], P('tp')
- k_cache: bfloat16 [4, 32768, 8, 128], P('dp', 'sp', 'tp')
- v_cache: bfloat16 [4, 32768, 8, 128], P('dp', 'sp', 'tp')
- positions: int32 [4], P('dp')
Outputs:
- output 1: bfloat16 [4, 8192], P('dp')
- output 2: bfloat16 [4, 32768, 8, 128], P('dp', 'sp', 'tp')
- output 3: bfloat16 [4, 32768, 8, 128], P('dp', 'sp', 'tp')
All inputs are finite; a program needn't handle non-finite values.
Results may differ from the reference program's by a relative error of at most 0.00424275.
Values sent between devices are 32-bit elements.
A program may use at most 1 GiB of HBM per device.

```python
import jax
import jax.numpy as jnp
from jax import lax

D = 8192
HEADS = 64
KV_HEADS = 8
HEAD = 128
BATCH = 4
SEQ = 32768
ROPE_BASE = 1000000
EPS = 1e-5
GROUP = HEADS // KV_HEADS


def rotary(tensor, positions):
    half_dim = tensor.shape[-1] // 2
    inv_freq = 1.0 / (ROPE_BASE ** (jnp.arange(half_dim, dtype=jnp.float32) * 2.0 / tensor.shape[-1]))
    angles = positions.astype(jnp.float32)[:, None, None] * inv_freq[None, None, :]
    cosine = jnp.cos(angles)
    sine_val = jnp.sin(angles)
    first_half = tensor[..., :half_dim]
    second_half = tensor[..., half_dim:]
    return jnp.concatenate([first_half * cosine - second_half * sine_val, first_half * sine_val + second_half * cosine], axis=-1)


def smooth_field(base_key, amplitude, noise_scale):
    key_coef, key_noise = jax.random.split(base_key)
    num_freq = 4
    seq_frac = jnp.arange(SEQ, dtype=jnp.float32) / SEQ
    freq_list = jnp.arange(1, num_freq + 1, dtype=jnp.float32)
    phases = 2.0 * jnp.pi * seq_frac[:, None] * freq_list[None, :]
    basis_mat = jnp.concatenate([jnp.cos(phases), jnp.sin(phases)], axis=1)
    coef_mat = jax.random.normal(key_coef, (BATCH, 2 * num_freq, KV_HEADS * HEAD), jnp.float32) * (amplitude / num_freq ** 0.5)
    smooth_part = jnp.einsum("sf,bfc->bsc", basis_mat, coef_mat)
    noise_part = jax.random.normal(key_noise, (BATCH, SEQ, KV_HEADS * HEAD), jnp.float32)
    return (smooth_part + noise_scale * noise_part).reshape(BATCH, SEQ, KV_HEADS, HEAD)


def draw_positions(base_key):
    key_len, key_pick = jax.random.split(base_key)
    pos_draw = jax.random.randint(key_len, (BATCH,), SEQ // 4, SEQ, jnp.int32)
    longest = jax.random.randint(key_pick, (), 0, BATCH, jnp.int32)
    return jnp.where(jnp.arange(BATCH) == longest, SEQ - 1, pos_draw).astype(jnp.int32)


def setup_inputs(seed: int = 0, part: int = 0) -> dict:
    key_list = jax.random.split(jax.random.key(seed), 9)
    q_width = HEADS * HEAD
    kv_width = KV_HEADS * HEAD
    norm_gain = 1.0 + 0.3 * jax.random.normal(key_list[0], (D,), jnp.float32)
    w_query32 = jax.random.normal(key_list[1], (D, q_width), jnp.float32) * D ** -0.5
    head_zero = w_query32.reshape(D, KV_HEADS, GROUP, HEAD)[:, :, 0, :].reshape(D, kv_width)
    w_key32 = 0.75 * head_zero + 0.66 * jax.random.normal(key_list[2], (D, kv_width), jnp.float32) * D ** -0.5
    w_value32 = jax.random.normal(key_list[3], (D, kv_width), jnp.float32) * D ** -0.5
    w_out32 = jax.random.normal(key_list[4], (q_width, D), jnp.float32) * q_width ** -0.5
    hidden = jax.random.normal(jax.random.fold_in(key_list[5], part), (BATCH, D), jnp.float32)
    k_cache = smooth_field(jax.random.fold_in(key_list[6], part), 1.2, 0.5)
    v_cache = smooth_field(jax.random.fold_in(key_list[7], part), 1.5, 0.5)
    positions = draw_positions(jax.random.fold_in(key_list[8], part))
    return {
        "hidden": hidden.astype(jnp.bfloat16),
        "norm_gain": norm_gain,
        "w_query": w_query32.astype(jnp.bfloat16),
        "w_key": w_key32.astype(jnp.bfloat16),
        "w_value": w_value32.astype(jnp.bfloat16),
        "w_out": w_out32.astype(jnp.bfloat16),
        "k_cache": k_cache.astype(jnp.bfloat16),
        "v_cache": v_cache.astype(jnp.bfloat16),
        "positions": positions,
    }


def reference(hidden, norm_gain, w_query, w_key, w_value, w_out, k_cache, v_cache, positions):
    resid_f32 = hidden.astype(jnp.float32)
    normed = (resid_f32 * lax.rsqrt(jnp.mean(resid_f32 * resid_f32, axis=-1, keepdims=True) + EPS) * norm_gain).astype(jnp.bfloat16)
    q_proj = jnp.dot(normed, w_query, preferred_element_type=jnp.float32).reshape(BATCH, HEADS, HEAD)
    k_proj = jnp.dot(normed, w_key, preferred_element_type=jnp.float32).reshape(BATCH, KV_HEADS, HEAD)
    v_new = jnp.dot(normed, w_value, preferred_element_type=jnp.float32).astype(jnp.bfloat16).reshape(BATCH, KV_HEADS, HEAD)
    q_rot = rotary(q_proj, positions).astype(jnp.bfloat16).reshape(BATCH, KV_HEADS, GROUP, HEAD)
    k_new = rotary(k_proj, positions).astype(jnp.bfloat16)
    slot_mask = (jnp.arange(SEQ)[None, :] == positions[:, None])[:, :, None, None]
    k_updated = jnp.where(slot_mask, k_new[:, None], k_cache)
    v_updated = jnp.where(slot_mask, v_new[:, None], v_cache)
    score_scale = HEAD ** -0.5

    def one_sequence(seq_args):
        q_seq, k_seq, v_seq, last_pos = seq_args
        scores = jnp.einsum("kgd,skd->kgs", q_seq.astype(jnp.float32), k_seq.astype(jnp.float32)) * score_scale
        scores = jnp.where(jnp.arange(SEQ) <= last_pos, scores, -jnp.inf)
        attn_prob = jax.nn.softmax(scores, axis=-1)
        return jnp.einsum("kgs,skd->kgd", attn_prob, v_seq.astype(jnp.float32))

    attn_out = lax.map(one_sequence, (q_rot, k_updated, v_updated, positions))
    attn_out = attn_out.astype(jnp.bfloat16).reshape(BATCH, HEADS * HEAD)
    proj_out = jnp.dot(attn_out, w_out, preferred_element_type=jnp.float32)
    return (resid_f32 + proj_out).astype(jnp.bfloat16), k_updated, v_updated
```

```python
import functools

import jax
import jax.numpy as jnp
import numpy as np
from jax import lax
from jax.experimental import pallas as pl
from jax.experimental.pallas import tpu as pltpu
from jax.sharding import PartitionSpec as P

ROPE_BASE = 1000000.0
EPS = 1e-5
NEG_BIG = -3.0e38
SIDE = 4
PLANE = SIDE * SIDE
AXES = ("x", "y", "z")
DIMS = (48, 40, 40)
STARTS = (0, 48, 88)
CHUNKS = 8
BF16 = jnp.bfloat16
F32 = jnp.float32


def sum_bytes(ref, sem):
    pltpu.make_async_copy(ref, ref, sem).wait()


def attention_kernel(
    hidden_hbm, gain_hbm, freq_hbm, pos_hbm, wq_hbm, wk_hbm, wv_hbm, wo_hbm, k_hbm, v_hbm,
    out_ref, knew_ref, vnew_ref,
    hid, gain, freq, wq, wk, wv, wo, kbuf, vbuf, gathered, fresh, rows, x0, x1, x2, orow, ypart, ypeer, yall,
    pos, sems, wq_sems, part_send, part_recv, qsend, qrecv, tpsend, tprecv, ysend, yrecv,
):
    batch, d_model = hid.shape
    head = 128
    seq_local = kbuf.shape[1] // 4
    me = lax.axis_index("sp")
    core = lax.axis_index("tp")
    lx = lax.rem(me, SIDE)
    ly = lax.rem(me // SIDE, SIDE)
    lz = me // PLANE
    cell = lax.rem(me, PLANE)
    line = {"x": lx, "y": ly, "z": lz}
    stride = {"x": 1, "y": SIDE, "z": PLANE}

    def line_peer(axis, step):
        here = line[axis]
        return me + (lax.rem(here + step, SIDE) - here) * stride[axis]

    def plane_peer(step_y, step_x):
        return lz * PLANE + lax.rem(ly + step_y, SIDE) * SIDE + lax.rem(lx + step_x, SIDE)

    plane_steps = sorted(
        [(a, b) for a in range(SIDE) for b in range(SIDE) if (a, b) != (0, 0)],
        key=lambda s: -(min(s[0], SIDE - s[0]) + min(s[1], SIDE - s[1])),
    )

    barrier = pltpu.get_barrier_semaphore()
    for a, b in plane_steps:
        pl.semaphore_signal(barrier, inc=1, device_id={"sp": plane_peer(a, b), "tp": core})
    for step in (2, 1, 3):
        pl.semaphore_signal(barrier, inc=1, device_id={"sp": line_peer("z", step), "tp": core})
    pl.semaphore_signal(barrier, inc=1, device_id={"sp": me, "tp": 1 - core})

    cp_hid = pltpu.make_async_copy(hidden_hbm, hid, sems.at[0])
    cp_gain = pltpu.make_async_copy(gain_hbm, gain, sems.at[1])
    cp_pos = pltpu.make_async_copy(pos_hbm, pos, sems.at[2])
    cp_freq = pltpu.make_async_copy(freq_hbm, freq, sems.at[3])
    for cp in (cp_hid, cp_gain, cp_pos, cp_freq):
        cp.start()
    q_cols = pl.ds(pl.multiple_of(cell * 256, 256), 256)
    q_rows = d_model // CHUNKS
    cp_wq = [
        pltpu.make_async_copy(
            wq_hbm.at[pl.ds(c * q_rows, q_rows), q_cols], wq.at[pl.ds(c * q_rows, q_rows), :], wq_sems.at[c]
        )
        for c in range(CHUNKS)
    ]
    kv_depth = d_model // SIDE
    kv_rows = pl.ds(pl.multiple_of(lx * kv_depth, kv_depth), kv_depth)
    kv_cols = pl.ds(pl.multiple_of(ly * head, head), head)
    cp_wk = pltpu.make_async_copy(wk_hbm.at[kv_rows, kv_cols], wk, sems.at[4])
    cp_wv = pltpu.make_async_copy(wv_hbm.at[kv_rows, kv_cols], wv, sems.at[5])
    for cp in cp_wq:
        cp.start()
    cp_wk.start()
    cp_wv.start()
    cp_k = pltpu.make_async_copy(k_hbm, kbuf, sems.at[6])
    cp_v = pltpu.make_async_copy(v_hbm, vbuf, sems.at[7])
    n_cols = wo.shape[1]
    o_cols = pl.ds(pl.multiple_of(cell * n_cols, n_cols), n_cols)
    cp_wo = pltpu.make_async_copy(wo_hbm.at[:, o_cols], wo, sems.at[8])

    cp_hid.wait()
    cp_gain.wait()
    resid = hid[...].astype(F32)
    scale = lax.rsqrt(jnp.mean(resid * resid, axis=-1, keepdims=True) + EPS)
    normed = (resid * scale * gain[...]).astype(BF16)

    cp_pos.wait()
    cp_freq.wait()
    row4 = lax.broadcasted_iota(jnp.int32, (batch, head), 0)
    lane4 = lax.broadcasted_iota(jnp.int32, (batch, head), 1)
    pos_rows = jnp.zeros((batch, head), jnp.int32)
    for b in range(batch):
        pos_rows = jnp.where(row4 == b, pos[b], pos_rows)
    angles = pos_rows.astype(F32) * freq[...]
    cosine = jnp.cos(angles)
    sine = jnp.sin(angles)
    sine = jnp.where(lane4 < head // 2, -sine, sine)

    def rotate(u):
        return u * cosine + pltpu.roll(u, head // 2, axis=1) * sine

    q_acc = jnp.zeros((batch, 256), F32)
    for c in range(CHUNKS):
        cp_wq[c].wait()
        q_acc += jnp.dot(
            normed[:, c * q_rows:(c + 1) * q_rows], wq[c * q_rows:(c + 1) * q_rows, :], preferred_element_type=F32
        )
    cp_k.start()
    cp_v.start()
    rows[...] = normed.astype(F32)
    normed_kv = rows[:, kv_rows].astype(BF16)
    cp_wk.wait()
    k_part = jnp.dot(normed_kv, wk[...], preferred_element_type=F32)
    cp_wv.wait()
    v_part = jnp.dot(normed_kv, wv[...], preferred_element_type=F32)
    q_lo = rotate(q_acc[:, :head]).astype(BF16).astype(F32)
    q_hi = rotate(q_acc[:, head:]).astype(BF16).astype(F32)
    mine = pl.ds(pl.multiple_of(cell * 16, 16), 16)
    gathered[mine, :] = jnp.concatenate([q_lo, q_hi, k_part, v_part], axis=0)

    pl.semaphore_wait(barrier, PLANE - 1 + SIDE - 1 + 1)
    for a, b in plane_steps:
        pltpu.make_async_remote_copy(
            src_ref=gathered.at[mine], dst_ref=gathered.at[mine], send_sem=qsend, recv_sem=qrecv,
            device_id={"sp": plane_peer(a, b), "tp": core},
        ).start()
    cp_wo.start()
    sum_bytes(gathered.at[pl.ds(0, 16 * (PLANE - 1))], qrecv)

    cos_all = jnp.concatenate([cosine] * 4, axis=0)
    sin_all = jnp.concatenate([sine] * 4, axis=0)
    k_sum, v_sum = [], []
    for j in range(4):
        k_sum.append(sum(gathered[(4 * j + i) * 16 + 8:(4 * j + i) * 16 + 12, :] for i in range(4)))
        v_sum.append(sum(gathered[(4 * j + i) * 16 + 12:(4 * j + i) * 16 + 16, :] for i in range(4)))
    k_all = jnp.concatenate(k_sum, axis=0)
    v_all = jnp.concatenate(v_sum, axis=0)
    k_all = k_all * cos_all + pltpu.roll(k_all, head // 2, axis=1) * sin_all
    fresh[0:16, :] = k_all.astype(BF16).astype(F32)
    fresh[16:32, :] = v_all.astype(BF16).astype(F32)

    cols = seq_local * 4
    row_head = lax.rem(lax.broadcasted_iota(jnp.int32, (32, cols), 0), 16) // 4
    col_id = lax.broadcasted_iota(jnp.int32, (32, cols), 1)
    same_head = row_head == lax.rem(col_id, 4)
    new_row = lax.rem(lax.broadcasted_iota(jnp.int32, (32, 16), 0), 16) // 4
    new_head = new_row == lax.broadcasted_iota(jnp.int32, (32, 16), 1)
    ones16 = lax.broadcasted_iota(jnp.int32, (32, 16), 1) * 0
    base = me * seq_local
    pad = jnp.zeros((12, head), F32)
    dims_last = (((1,), (1,)), ((), ()))
    cp_k.wait()
    cp_v.wait()
    acc_rows, m_rows, l_rows = [], [], []
    for b in range(batch):
        k_b = jnp.concatenate([fresh[pl.ds(b, 4, stride=4), :], pad], axis=0).astype(BF16)
        v_b = jnp.concatenate([fresh[pl.ds(16 + b, 4, stride=4), :], pad], axis=0).astype(BF16)
        knew_ref[b] = k_b[0:4]
        vnew_ref[b] = v_b[0:4]
        q_b = jnp.concatenate(
            [gathered[pl.ds(b, 16, stride=16), :], gathered[pl.ds(4 + b, 16, stride=16), :]], axis=0
        ).astype(BF16)
        limit = (pos[b] - base) * 4
        valid = jnp.logical_and(same_head, col_id < limit)
        valid_new = jnp.logical_and(
            new_head, jnp.logical_and(ones16 + limit >= 0, ones16 + limit < cols)
        )
        s = lax.dot_general(q_b, kbuf[b], dims_last, preferred_element_type=F32) * (head ** -0.5)
        s_new = lax.dot_general(q_b, k_b, dims_last, preferred_element_type=F32) * (head ** -0.5)
        s = jnp.where(valid, s, NEG_BIG)
        s_new = jnp.where(valid_new, s_new, NEG_BIG)
        m = jnp.maximum(jnp.max(s, axis=-1, keepdims=True), jnp.max(s_new, axis=-1, keepdims=True))
        p = jnp.where(valid, jnp.exp(s - m), 0.0)
        p_new = jnp.where(valid_new, jnp.exp(s_new - m), 0.0)
        l_rows.append(jnp.sum(p, axis=-1, keepdims=True) + jnp.sum(p_new, axis=-1, keepdims=True))
        m_rows.append(m)
        acc_rows.append(
            jnp.dot(p.astype(BF16), vbuf[b], preferred_element_type=F32)
            + jnp.dot(p_new.astype(BF16), v_b, preferred_element_type=F32)
        )
    acc_t = jnp.concatenate(acc_rows, axis=0).T
    m_col = jnp.concatenate(m_rows, axis=0)
    l_col = jnp.concatenate(l_rows, axis=0)
    lane = lax.broadcasted_iota(jnp.int32, (128, 128), 1)
    stat_t = jnp.where(lane == 0, m_col, l_col).T[0:8]

    parts = (x0, x1, x2)

    def send_part(p, t):
        axis = AXES[(p + t) % 3]
        slot = parts[p].at[t, line[axis]]
        for step in (2, 1, 3):
            pltpu.make_async_remote_copy(
                src_ref=slot, dst_ref=slot, send_sem=part_send.at[p, t], recv_sem=part_recv.at[p, t],
                device_id={"sp": line_peer(axis, step), "tp": core},
            ).start()

    for p in range(3):
        axis = AXES[p]
        parts[p][0, line[axis], 0:DIMS[p], :] = acc_t[STARTS[p]:STARTS[p] + DIMS[p]]
        parts[p][0, line[axis], DIMS[p]:DIMS[p] + 8, :] = stat_t
    for p in range(3):
        send_part(p, 0)
    o_parts = []
    for t in range(3):
        for p in range(3):
            ref = parts[p]
            sum_bytes(ref.at[t, pl.ds(0, SIDE - 1)], part_recv.at[p, t])
            stats = [ref[t, i, DIMS[p]:DIMS[p] + 8, :] for i in range(SIDE)]
            ms = [st[0:1] for st in stats]
            top = jnp.maximum(jnp.maximum(ms[0], ms[1]), jnp.maximum(ms[2], ms[3]))
            fac = [jnp.exp(mi - top) for mi in ms]
            acc = sum(ref[t, i, 0:DIMS[p], :] * fac[i] for i in range(SIDE))
            total = sum(stats[i][1:2] * fac[i] for i in range(SIDE))
            if t < 2:
                slot = line[AXES[(p + t + 1) % 3]]
                ref[t + 1, slot, 0:DIMS[p], :] = acc
                row8 = lax.broadcasted_iota(jnp.int32, (8, 128), 0)
                ref[t + 1, slot, DIMS[p]:DIMS[p] + 8, :] = jnp.where(row8 == 0, top, total)
                send_part(p, t + 1)
            else:
                o_parts.append(acc / total)
    orow[...] = jnp.concatenate(o_parts, axis=0).T

    attn = jnp.concatenate(
        [orow[pl.ds(h // 2 + 16 * (h % 2), batch, stride=32), :] for h in range(32)], axis=1
    ).astype(BF16)
    cp_wo.wait()
    o_rows = wo.shape[0] // CHUNKS
    y = jnp.zeros((batch, n_cols), F32)
    for c in range(CHUNKS):
        y += jnp.dot(
            attn[:, c * o_rows:(c + 1) * o_rows], wo[c * o_rows:(c + 1) * o_rows, :], preferred_element_type=F32
        )
    ypart[...] = y
    cp_tp = pltpu.make_async_remote_copy(
        src_ref=ypart, dst_ref=ypeer, send_sem=tpsend, recv_sem=tprecv, device_id={"sp": me, "tp": 1 - core}
    )
    cp_tp.start()
    cp_tp.wait_recv()
    yall[cell] = ypart[...] + ypeer[...]
    for a, b in plane_steps:
        pltpu.make_async_remote_copy(
            src_ref=yall.at[cell], dst_ref=yall.at[cell], send_sem=ysend, recv_sem=yrecv,
            device_id={"sp": plane_peer(a, b), "tp": core},
        ).start()
    sum_bytes(yall.at[pl.ds(0, PLANE - 1)], yrecv)
    for i in range(PLANE):
        out_ref[:, i * n_cols:(i + 1) * n_cols] = (
            hid[:, i * n_cols:(i + 1) * n_cols].astype(F32) + yall[i]
        ).astype(BF16)

    cp_tp.wait_send()
    sum_bytes(gathered.at[pl.ds(0, 16 * (PLANE - 1))], qsend)
    sum_bytes(yall.at[pl.ds(0, PLANE - 1)], ysend)
    for t in range(3):
        for p in range(3):
            sum_bytes(parts[p].at[t, pl.ds(0, SIDE - 1)], part_send.at[p, t])


def update_kernel(base_unused, y_ref, k_ref, v_ref, knew_ref, vnew_ref, pos_ref, out_ref, ko_ref, vo_ref, sems, row_sems):
    batch, seq_local = k_ref.shape[0], k_ref.shape[1]
    base = lax.axis_index("sp") * seq_local
    bulk = []
    for b in range(batch):
        bulk.append(pltpu.make_async_copy(k_ref.at[b], ko_ref.at[b], sems.at[0, b]))
        bulk.append(pltpu.make_async_copy(v_ref.at[b], vo_ref.at[b], sems.at[1, b]))
    for cp in bulk:
        cp.start()
    out_ref[...] = y_ref[...]
    for b in range(batch):
        bulk[2 * b].wait()
        bulk[2 * b + 1].wait()
        spot = pos_ref[b] - base

        @pl.when(jnp.logical_and(spot >= 0, spot < seq_local))
        def _():
            cp_k = pltpu.make_async_copy(knew_ref.at[b], ko_ref.at[b, spot], row_sems.at[0])
            cp_v = pltpu.make_async_copy(vnew_ref.at[b], vo_ref.at[b, spot], row_sems.at[1])
            cp_k.start()
            cp_v.start()
            cp_k.wait()
            cp_v.wait()


def solution(mesh):
    def local_step(hidden, norm_gain, w_query, w_key, w_value, w_out, k_cache, v_cache, positions):
        batch, seq_local, kv_local, head = k_cache.shape
        d_model = hidden.shape[1]
        n_cols = w_out.shape[1] // PLANE
        half = np.arange(head // 2, dtype=np.float32) * np.float32(2.0) / np.float32(head)
        inv = (np.float32(1.0) / np.power(np.float32(ROPE_BASE), half)).astype(np.float32)
        freq = jnp.asarray(np.concatenate([inv, inv])[None, :])
        flat = (batch, seq_local * kv_local, head)
        hbm = pl.BlockSpec(memory_space=pltpu.HBM)
        vmem = pl.BlockSpec(memory_space=pltpu.VMEM)
        dma = pltpu.SemaphoreType.DMA
        y, k_new, v_new = pl.pallas_call(
            attention_kernel,
            out_shape=[
                jax.ShapeDtypeStruct(hidden.shape, BF16),
                jax.ShapeDtypeStruct((batch, kv_local, head), BF16),
                jax.ShapeDtypeStruct((batch, kv_local, head), BF16),
            ],
            in_specs=[hbm] * 10,
            out_specs=[vmem] * 3,
            scratch_shapes=[
                pltpu.VMEM(hidden.shape, BF16),
                pltpu.VMEM((1, d_model), F32),
                pltpu.VMEM((1, head), F32),
                pltpu.VMEM((d_model, 256), BF16),
                pltpu.VMEM((d_model // SIDE, head), BF16),
                pltpu.VMEM((d_model // SIDE, head), BF16),
                pltpu.VMEM((w_out.shape[0], n_cols), BF16),
                pltpu.VMEM(flat, BF16),
                pltpu.VMEM(flat, BF16),
                pltpu.VMEM((PLANE * 16, head), F32),
                pltpu.VMEM((32, head), F32),
                pltpu.VMEM((batch, d_model), F32),
                *[pltpu.VMEM((3, SIDE, d + 8, 128), F32) for d in DIMS],
                pltpu.VMEM((128, 128), F32),
                pltpu.VMEM((batch, n_cols), F32),
                pltpu.VMEM((batch, n_cols), F32),
                pltpu.VMEM((PLANE, batch, n_cols), F32),
                pltpu.SMEM((batch,), jnp.int32),
                dma((9,)),
                dma((CHUNKS,)),
                dma((3, 3)),
                dma((3, 3)),
                dma, dma, dma, dma, dma, dma,
            ],
            compiler_params=pltpu.CompilerParams(
                collective_id=0, has_side_effects=True, vmem_limit_bytes=30 << 20
            ),
            cost_estimate=pl.CostEstimate(flops=20_000_000_000, bytes_accessed=20_000_000, transcendentals=0),
            name="attention_step",
        )(
            hidden, norm_gain.reshape(1, d_model), freq, positions, w_query, w_key, w_value, w_out,
            k_cache.reshape(flat), v_cache.reshape(flat),
        )
        any_space = pl.BlockSpec(memory_space=pl.ANY)
        return pl.pallas_call(
            functools.partial(update_kernel, None),
            out_shape=[
                jax.ShapeDtypeStruct(hidden.shape, BF16),
                jax.ShapeDtypeStruct(k_cache.shape, BF16),
                jax.ShapeDtypeStruct(v_cache.shape, BF16),
            ],
            in_specs=[vmem] * 5 + [pl.BlockSpec(memory_space=pltpu.SMEM)],
            out_specs=[vmem, any_space, any_space],
            scratch_shapes=[dma((2, batch)), dma((2,))],
            compiler_params=pltpu.CompilerParams(vmem_limit_bytes=16 << 20),
            cost_estimate=pl.CostEstimate(flops=1_000_000, bytes_accessed=8_000_000, transcendentals=0),
            name="cache_update",
        )(y, k_cache, v_cache, k_new, v_new, positions)

    cache_spec = P("dp", "sp", "tp", None)
    specs_in = (P("dp", None), P(None), P(None, "tp"), P(None, "tp"), P(None, "tp"), P("tp", None), cache_spec, cache_spec, P("dp"))
    specs_out = (P("dp", None), cache_spec, cache_spec)
    return jax.shard_map(local_step, mesh=mesh, in_specs=specs_in, out_specs=specs_out, check_vma=False)
```

```python
import jax
import jax.numpy as jnp
import numpy as np
from jax import lax
from jax.experimental import pallas as pl
from jax.experimental.pallas import tpu as pltpu
from jax.sharding import PartitionSpec as P

ROPE_BASE = 1000000.0
EPS = 1e-5
NEG_BIG = -3.0e38
SIDE = 4
PLANE = SIDE * SIDE
AXES = ("x", "y", "z")
PARTS = ((0, 24, True), (1, 24, True), (2, 24, True), (0, 24, False), (1, 16, False), (2, 16, False))
STARTS = tuple(sum(d for _, d, _ in PARTS[:i]) for i in range(len(PARTS)))
HALVES = 2
CHUNKS = 8
BF16 = jnp.bfloat16
F32 = jnp.float32


def sum_bytes(ref, sem):
    pltpu.make_async_copy(ref, ref, sem).wait()


def attention_kernel(
    hidden_hbm, gain_hbm, freq_hbm, pos_hbm, wq_hbm, wk_hbm, wv_hbm, wo_hbm, k_hbm, v_hbm,
    out_ref, knew_ref, vnew_ref,
    hid, gain, freq, wq, wk, wv, wo, kbuf, vbuf, kturn, gathered, fresh, rows, x0, x1, x2, x3, x4, x5, orow,
    ypart, ypeer, yall, pos, sems, wq_sems, part_send, part_recv, qsend, qrecv, tpsend, tprecv, ysend, yrecv,
):
    batch, d_model = hid.shape
    head = 128
    seq_local = kbuf.shape[1] // 4
    me = lax.axis_index("sp")
    core = lax.axis_index("tp")
    lx = lax.rem(me, SIDE)
    ly = lax.rem(me // SIDE, SIDE)
    lz = me // PLANE
    cell = lax.rem(me, PLANE)
    line = {"x": lx, "y": ly, "z": lz}
    stride = {"x": 1, "y": SIDE, "z": PLANE}

    def line_peer(axis, step):
        here = line[axis]
        return me + (lax.rem(here + step, SIDE) - here) * stride[axis]

    def plane_peer(step_y, step_x):
        return lz * PLANE + lax.rem(ly + step_y, SIDE) * SIDE + lax.rem(lx + step_x, SIDE)

    plane_steps = sorted(
        [(a, b) for a in range(SIDE) for b in range(SIDE) if (a, b) != (0, 0)],
        key=lambda s: -(min(s[0], SIDE - s[0]) + min(s[1], SIDE - s[1])),
    )

    cp_hid = pltpu.make_async_copy(hidden_hbm, hid, sems.at[0])
    cp_gain = pltpu.make_async_copy(gain_hbm, gain, sems.at[1])
    cp_pos = pltpu.make_async_copy(pos_hbm, pos, sems.at[2])
    cp_freq = pltpu.make_async_copy(freq_hbm, freq, sems.at[3])
    for cp in (cp_hid, cp_gain, cp_pos, cp_freq):
        cp.start()
    q_cols = pl.ds(pl.multiple_of(cell * 256, 256), 256)
    q_rows = d_model // CHUNKS
    cp_wq = [
        pltpu.make_async_copy(
            wq_hbm.at[pl.ds(c * q_rows, q_rows), q_cols], wq.at[pl.ds(c * q_rows, q_rows), :], wq_sems.at[c]
        )
        for c in range(CHUNKS)
    ]
    kv_depth = d_model // SIDE
    kv_rows = pl.ds(pl.multiple_of(lx * kv_depth, kv_depth), kv_depth)
    kv_cols = pl.ds(pl.multiple_of(ly * head, head), head)
    cp_wk = pltpu.make_async_copy(wk_hbm.at[kv_rows, kv_cols], wk, sems.at[4])
    cp_wv = pltpu.make_async_copy(wv_hbm.at[kv_rows, kv_cols], wv, sems.at[5])
    cp_wk.start()
    cp_wv.start()
    for cp in cp_wq:
        cp.start()
    cp_k = pltpu.make_async_copy(k_hbm, kbuf, sems.at[6])
    cp_v = pltpu.make_async_copy(v_hbm, vbuf, sems.at[7])
    n_cols = wo.shape[1]
    o_cols = pl.ds(pl.multiple_of(cell * n_cols, n_cols), n_cols)
    cp_wo = pltpu.make_async_copy(wo_hbm.at[:, o_cols], wo, sems.at[8])

    barrier = pltpu.get_barrier_semaphore()
    for a, b in plane_steps:
        pl.semaphore_signal(barrier, inc=1, device_id={"sp": plane_peer(a, b), "tp": core})
    for step in (2, 1, 3):
        pl.semaphore_signal(barrier, inc=1, device_id={"sp": line_peer("z", step), "tp": core})
    pl.semaphore_signal(barrier, inc=1, device_id={"sp": me, "tp": 1 - core})

    cp_hid.wait()
    cp_gain.wait()
    resid = hid[...].astype(F32)
    scale = lax.rsqrt(jnp.mean(resid * resid, axis=-1, keepdims=True) + EPS)
    normed = (resid * scale * gain[...]).astype(BF16)

    rows[...] = normed.astype(F32)
    normed_kv = rows[:, kv_rows].astype(BF16)
    cp_wk.wait()
    cp_wv.wait()
    k_part = jnp.dot(normed_kv, wk[...], preferred_element_type=F32)
    v_part = jnp.dot(normed_kv, wv[...], preferred_element_type=F32)
    q_acc = jnp.zeros((batch, 256), F32)
    for c in range(CHUNKS):
        if c == 2:
            cp_pos.wait()
            cp_freq.wait()
            row4 = lax.broadcasted_iota(jnp.int32, (batch, head), 0)
            lane4 = lax.broadcasted_iota(jnp.int32, (batch, head), 1)
            pos_rows = jnp.zeros((batch, head), jnp.int32)
            for b in range(batch):
                pos_rows = jnp.where(row4 == b, pos[b], pos_rows)
            angles = pos_rows.astype(F32) * freq[...]
            cosine = jnp.cos(angles)
            sine = jnp.sin(angles)
            sine = jnp.where(lane4 < head // 2, -sine, sine)
        cp_wq[c].wait()
        q_acc += jnp.dot(
            normed[:, c * q_rows:(c + 1) * q_rows], wq[c * q_rows:(c + 1) * q_rows, :], preferred_element_type=F32
        )
    cp_k.start()
    cp_v.start()

    def rotate(u):
        return u * cosine + pltpu.roll(u, head // 2, axis=1) * sine

    q_lo = rotate(q_acc[:, :head]).astype(BF16).astype(F32)
    q_hi = rotate(q_acc[:, head:]).astype(BF16).astype(F32)
    mine = pl.ds(pl.multiple_of(cell * 16, 16), 16)
    gathered[mine, :] = jnp.concatenate([q_lo, q_hi, k_part, v_part], axis=0)

    pl.semaphore_wait(barrier, PLANE - 1 + SIDE - 1 + 1)
    for a, b in plane_steps:
        pltpu.make_async_remote_copy(
            src_ref=gathered.at[mine], dst_ref=gathered.at[mine], send_sem=qsend, recv_sem=qrecv,
            device_id={"sp": plane_peer(a, b), "tp": core},
        ).start()
    cp_wo.start()
    cp_k.wait()
    for b in range(batch):
        kturn[b] = kbuf[b].T
    sum_bytes(gathered.at[pl.ds(0, 16 * (PLANE - 1))], qrecv)

    cos_all = jnp.concatenate([cosine] * 4, axis=0)
    sin_all = jnp.concatenate([sine] * 4, axis=0)
    k_sum, v_sum = [], []
    for j in range(4):
        k_sum.append(sum(gathered[(4 * j + i) * 16 + 8:(4 * j + i) * 16 + 12, :] for i in range(4)))
        v_sum.append(sum(gathered[(4 * j + i) * 16 + 12:(4 * j + i) * 16 + 16, :] for i in range(4)))
    k_all = jnp.concatenate(k_sum, axis=0)
    v_all = jnp.concatenate(v_sum, axis=0)
    k_all = k_all * cos_all + pltpu.roll(k_all, head // 2, axis=1) * sin_all
    fresh[0:16, :] = k_all.astype(BF16).astype(F32)
    fresh[16:32, :] = v_all.astype(BF16).astype(F32)

    cols = seq_local * 4
    row_head = lax.rem(lax.broadcasted_iota(jnp.int32, (32, cols), 0), 16) // 4
    col_id = lax.broadcasted_iota(jnp.int32, (32, cols), 1)
    same_head = row_head == lax.rem(col_id, 4)
    new_row = lax.rem(lax.broadcasted_iota(jnp.int32, (32, 16), 0), 16) // 4
    new_head = new_row == lax.broadcasted_iota(jnp.int32, (32, 16), 1)
    ones16 = lax.broadcasted_iota(jnp.int32, (32, 16), 1) * 0
    base = me * seq_local
    pad = jnp.zeros((12, head), F32)
    dims_last = (((1,), (1,)), ((), ()))
    cp_v.wait()
    acc_rows, m_rows, l_rows = [], [], []
    for b in range(batch):
        k_b = jnp.concatenate([fresh[pl.ds(b, 4, stride=4), :], pad], axis=0).astype(BF16)
        v_b = jnp.concatenate([fresh[pl.ds(16 + b, 4, stride=4), :], pad], axis=0).astype(BF16)
        knew_ref[b, 0] = k_b[0:4]
        vnew_ref[b, 0] = v_b[0:4]
        q_b = jnp.concatenate(
            [gathered[pl.ds(b, 16, stride=16), :], gathered[pl.ds(4 + b, 16, stride=16), :]], axis=0
        ).astype(BF16)
        limit = (pos[b] - base) * 4
        valid = jnp.logical_and(same_head, col_id < limit)
        valid_new = jnp.logical_and(
            new_head, jnp.logical_and(ones16 + limit >= 0, ones16 + limit < cols)
        )
        s = jnp.dot(q_b, kturn[b], preferred_element_type=F32) * (head ** -0.5)
        s_new = lax.dot_general(q_b, k_b, dims_last, preferred_element_type=F32) * (head ** -0.5)
        s = jnp.where(valid, s, NEG_BIG)
        s_new = jnp.where(valid_new, s_new, NEG_BIG)
        m = jnp.maximum(jnp.max(s, axis=-1, keepdims=True), jnp.max(s_new, axis=-1, keepdims=True))
        p = jnp.where(valid, jnp.exp(s - m), 0.0)
        p_new = jnp.where(valid_new, jnp.exp(s_new - m), 0.0)
        l_rows.append(jnp.sum(p, axis=-1, keepdims=True) + jnp.sum(p_new, axis=-1, keepdims=True))
        m_rows.append(m)
        acc_rows.append(
            jnp.dot(p.astype(BF16), vbuf[b], preferred_element_type=F32)
            + jnp.dot(p_new.astype(BF16), v_b, preferred_element_type=F32)
        )
    acc_t = jnp.concatenate(acc_rows, axis=0).T
    m_col = jnp.concatenate(m_rows, axis=0)
    l_col = jnp.concatenate(l_rows, axis=0)
    lane = lax.broadcasted_iota(jnp.int32, (128, 128), 1)
    stat_t = jnp.where(lane == 0, m_col, l_col).T[0:8]

    parts = (x0, x1, x2, x3, x4, x5)

    def send_part(p, t):
        axis = AXES[(PARTS[p][0] + t) % 3]
        slot = parts[p].at[t, line[axis]]
        for step in (2, 1, 3):
            pltpu.make_async_remote_copy(
                src_ref=slot, dst_ref=slot, send_sem=part_send.at[p, t], recv_sem=part_recv.at[p, t],
                device_id={"sp": line_peer(axis, step), "tp": core},
            ).start()

    for p, (order, dims, has_stats) in enumerate(PARTS):
        slot = line[AXES[order]]
        parts[p][0, slot, 0:dims, :] = acc_t[STARTS[p]:STARTS[p] + dims]
        if has_stats:
            parts[p][0, slot, dims:dims + 8, :] = stat_t
        send_part(p, 0)
    o_parts = []
    row8 = lax.broadcasted_iota(jnp.int32, (8, 128), 0)
    factors = {}
    for t in range(3):
        for p, (order, dims, has_stats) in enumerate(PARTS):
            ref = parts[p]
            sum_bytes(ref.at[t, pl.ds(0, SIDE - 1)], part_recv.at[p, t])
            if has_stats:
                stats = [ref[t, i, dims:dims + 8, :] for i in range(SIDE)]
                ms = [st[0:1] for st in stats]
                top = jnp.maximum(jnp.maximum(ms[0], ms[1]), jnp.maximum(ms[2], ms[3]))
                fac = [jnp.exp(mi - top) for mi in ms]
                total = sum(stats[i][1:2] * fac[i] for i in range(SIDE))
                factors[order] = (fac, total)
            fac, total = factors[order]
            acc = sum(ref[t, i, 0:dims, :] * fac[i] for i in range(SIDE))
            if t < 2:
                slot = line[AXES[(order + t + 1) % 3]]
                ref[t + 1, slot, 0:dims, :] = acc
                if has_stats:
                    ref[t + 1, slot, dims:dims + 8, :] = jnp.where(row8 == 0, top, total)
                send_part(p, t + 1)
            else:
                o_parts.append(acc / total)
    orow[...] = jnp.concatenate(o_parts, axis=0).T

    attn = jnp.concatenate(
        [orow[pl.ds(h // 2 + 16 * (h % 2), batch, stride=32), :] for h in range(32)], axis=1
    ).astype(BF16)
    cp_wo.wait()
    o_rows = wo.shape[0] // CHUNKS
    half = n_cols // HALVES
    cp_tp = []
    for u in range(HALVES):
        y = jnp.zeros((batch, half), F32)
        for c in range(CHUNKS):
            y += jnp.dot(
                attn[:, c * o_rows:(c + 1) * o_rows],
                wo[c * o_rows:(c + 1) * o_rows, u * half:(u + 1) * half],
                preferred_element_type=F32,
            )
        ypart[u] = y
        cp_tp.append(
            pltpu.make_async_remote_copy(
                src_ref=ypart.at[u], dst_ref=ypeer.at[u], send_sem=tpsend.at[u], recv_sem=tprecv.at[u],
                device_id={"sp": me, "tp": 1 - core},
            )
        )
        cp_tp[u].start()
    for u in range(HALVES):
        cp_tp[u].wait_recv()
        yall[u, cell] = ypart[u] + ypeer[u]
        for a, b in plane_steps:
            pltpu.make_async_remote_copy(
                src_ref=yall.at[u, cell], dst_ref=yall.at[u, cell], send_sem=ysend.at[u], recv_sem=yrecv.at[u],
                device_id={"sp": plane_peer(a, b), "tp": core},
            ).start()

    sum_bytes(gathered.at[pl.ds(0, 16 * (PLANE - 1))], qsend)
    for t in range(3):
        for p in range(len(PARTS)):
            sum_bytes(parts[p].at[t, pl.ds(0, SIDE - 1)], part_send.at[p, t])
    for u in range(HALVES):
        cp_tp[u].wait_send()

    for u in range(HALVES):
        sum_bytes(yall.at[u, pl.ds(0, PLANE - 1)], yrecv.at[u])
        for i in range(PLANE):
            lo = i * n_cols + u * half
            out_ref[:, lo:lo + half] = (hid[:, lo:lo + half].astype(F32) + yall[u, i]).astype(BF16)
    for u in range(HALVES):
        sum_bytes(yall.at[u, pl.ds(0, PLANE - 1)], ysend.at[u])


def update_kernel(y_ref, k_ref, v_ref, knew_ref, vnew_ref, pos_ref, out_ref, ko_ref, vo_ref, y_sem, sems):
    batch, seq_local = k_ref.shape[0], k_ref.shape[1]
    base = lax.axis_index("sp") * seq_local
    copies = [pltpu.make_async_copy(y_ref, out_ref, y_sem)]
    for b in range(batch):
        spot = pos_ref[b] - base
        here = jnp.logical_and(spot >= 0, spot < seq_local).astype(jnp.int32)
        before = here * spot + (1 - here) * seq_local
        spot = here * spot
        after = here * (seq_local - 1 - spot)
        tail = pl.ds(seq_local - after, after)
        for i, (src, new, dst) in enumerate(((k_ref, knew_ref, ko_ref), (v_ref, vnew_ref, vo_ref))):
            head_rows = pl.ds(0, before)
            row = pl.ds(spot, here)
            copies.append(pltpu.make_async_copy(src.at[b, head_rows], dst.at[b, head_rows], sems.at[i, b, 0]))
            copies.append(pltpu.make_async_copy(src.at[b, tail], dst.at[b, tail], sems.at[i, b, 1]))
            copies.append(pltpu.make_async_copy(new.at[b, pl.ds(0, here)], dst.at[b, row], sems.at[i, b, 2]))
    for cp in copies:
        cp.start()
    for cp in copies:
        cp.wait()


def solution(mesh):
    def local_step(hidden, norm_gain, w_query, w_key, w_value, w_out, k_cache, v_cache, positions):
        batch, seq_local, kv_local, head = k_cache.shape
        d_model = hidden.shape[1]
        n_cols = w_out.shape[1] // PLANE
        half = np.arange(head // 2, dtype=np.float32) * np.float32(2.0) / np.float32(head)
        inv = (np.float32(1.0) / np.power(np.float32(ROPE_BASE), half)).astype(np.float32)
        freq = jnp.asarray(np.concatenate([inv, inv])[None, :])
        flat = (batch, seq_local * kv_local, head)
        hbm = pl.BlockSpec(memory_space=pltpu.HBM)
        vmem = pl.BlockSpec(memory_space=pltpu.VMEM)
        dma = pltpu.SemaphoreType.DMA
        y, k_new, v_new = pl.pallas_call(
            attention_kernel,
            out_shape=[
                jax.ShapeDtypeStruct(hidden.shape, BF16),
                jax.ShapeDtypeStruct((batch, 1, kv_local, head), BF16),
                jax.ShapeDtypeStruct((batch, 1, kv_local, head), BF16),
            ],
            in_specs=[hbm] * 10,
            out_specs=[vmem] * 3,
            scratch_shapes=[
                pltpu.VMEM(hidden.shape, BF16),
                pltpu.VMEM((1, d_model), F32),
                pltpu.VMEM((1, head), F32),
                pltpu.VMEM((d_model, 256), BF16),
                pltpu.VMEM((d_model // SIDE, head), BF16),
                pltpu.VMEM((d_model // SIDE, head), BF16),
                pltpu.VMEM((w_out.shape[0], n_cols), BF16),
                pltpu.VMEM(flat, BF16),
                pltpu.VMEM(flat, BF16),
                pltpu.VMEM((batch, head, seq_local * kv_local), BF16),
                pltpu.VMEM((PLANE * 16, head), F32),
                pltpu.VMEM((32, head), F32),
                pltpu.VMEM((batch, d_model), F32),
                *[pltpu.VMEM((3, SIDE, d + 8 * stats, 128), F32) for _, d, stats in PARTS],
                pltpu.VMEM((128, 128), F32),
                pltpu.VMEM((HALVES, batch, n_cols // HALVES), F32),
                pltpu.VMEM((HALVES, batch, n_cols // HALVES), F32),
                pltpu.VMEM((HALVES, PLANE, batch, n_cols // HALVES), F32),
                pltpu.SMEM((batch,), jnp.int32),
                dma((9,)),
                dma((CHUNKS,)),
                dma((len(PARTS), 3)),
                dma((len(PARTS), 3)),
                dma, dma,
                *[dma((HALVES,))] * 4,
            ],
            compiler_params=pltpu.CompilerParams(
                collective_id=0, has_side_effects=True, vmem_limit_bytes=30 << 20
            ),
            cost_estimate=pl.CostEstimate(flops=20_000_000_000, bytes_accessed=20_000_000, transcendentals=0),
            name="attention_step",
        )(
            *[
                pltpu.with_memory_space_constraint(a, pltpu.HBM)
                for a in (
                    hidden, norm_gain.reshape(1, d_model), freq, positions, w_query, w_key, w_value, w_out,
                    k_cache.reshape(flat), v_cache.reshape(flat),
                )
            ]
        )
        any_space = pl.BlockSpec(memory_space=pl.ANY)
        return pl.pallas_call(
            update_kernel,
            out_shape=[
                jax.ShapeDtypeStruct(hidden.shape, BF16),
                jax.ShapeDtypeStruct(k_cache.shape, BF16),
                jax.ShapeDtypeStruct(v_cache.shape, BF16),
            ],
            in_specs=[vmem] * 5 + [pl.BlockSpec(memory_space=pltpu.SMEM)],
            out_specs=[any_space] * 3,
            scratch_shapes=[dma, dma((2, batch, 3))],
            compiler_params=pltpu.CompilerParams(vmem_limit_bytes=16 << 20),
            cost_estimate=pl.CostEstimate(flops=1_000_000, bytes_accessed=8_000_000, transcendentals=0),
            name="cache_update",
        )(y, k_cache, v_cache, k_new, v_new, positions)

    cache_spec = P("dp", "sp", "tp", None)
    specs_in = (P("dp", None), P(None), P(None, "tp"), P(None, "tp"), P(None, "tp"), P("tp", None), cache_spec, cache_spec, P("dp"))
    specs_out = (P("dp", None), cache_spec, cache_spec)
    return jax.shard_map(local_step, mesh=mesh, in_specs=specs_in, out_specs=specs_out, check_vma=False)
```

```python
import jax
import jax.numpy as jnp
import numpy as np
from jax import lax
from jax.experimental import pallas as pl
from jax.experimental.pallas import tpu as pltpu
from jax.sharding import PartitionSpec as P

ROPE_BASE = 1000000.0
EPS = 1e-5
NEG_BIG = -3.0e38
SIDE = 4
PLANE = SIDE * SIDE
AXES = ("x", "y", "z")
PARTS = (
    (0, 16, True), (1, 16, True), (2, 16, True),
    (0, 16, False), (1, 16, False), (2, 16, False),
    (0, 16, False), (1, 8, False), (2, 8, False),
)
STARTS = tuple(sum(d for _, d, _ in PARTS[:i]) for i in range(len(PARTS)))
HALVES = 2
CHUNKS = 8
BF16 = jnp.bfloat16
F32 = jnp.float32


def sum_bytes(ref, sem):
    pltpu.make_async_copy(ref, ref, sem).wait()


def attention_kernel(
    hidden_hbm, gain_hbm, freq_hbm, pos_hbm, wq_hbm, wk_hbm, wv_hbm, wo_hbm, k_hbm, v_hbm,
    out_ref, kbuf, vbuf,
    hid, gain, freq, wq, wk, wv, wo, kturn, gathered, fresh, rows, x0, x1, x2, x3, x4, x5, x6, x7, x8, orow,
    ypart, ypeer, yall, pos, sems, wq_sems, part_send, part_recv, qsend, qrecv, tpsend, tprecv, ysend, yrecv,
):
    batch, d_model = hid.shape
    head = 128
    seq_local = kbuf.shape[1] // 4
    me = lax.axis_index("sp")
    core = lax.axis_index("tp")
    lx = lax.rem(me, SIDE)
    ly = lax.rem(me // SIDE, SIDE)
    lz = me // PLANE
    cell = lax.rem(me, PLANE)
    line = {"x": lx, "y": ly, "z": lz}
    stride = {"x": 1, "y": SIDE, "z": PLANE}

    def line_peer(axis, step):
        here = line[axis]
        return me + (lax.rem(here + step, SIDE) - here) * stride[axis]

    def plane_peer(step_y, step_x):
        return lz * PLANE + lax.rem(ly + step_y, SIDE) * SIDE + lax.rem(lx + step_x, SIDE)

    plane_steps = sorted(
        [(a, b) for a in range(SIDE) for b in range(SIDE) if (a, b) != (0, 0)],
        key=lambda s: -(min(s[0], SIDE - s[0]) + min(s[1], SIDE - s[1])),
    )

    cp_hid = pltpu.make_async_copy(hidden_hbm, hid, sems.at[0])
    cp_gain = pltpu.make_async_copy(gain_hbm, gain, sems.at[1])
    cp_pos = pltpu.make_async_copy(pos_hbm, pos, sems.at[2])
    cp_freq = pltpu.make_async_copy(freq_hbm, freq, sems.at[3])
    for cp in (cp_hid, cp_gain, cp_pos, cp_freq):
        cp.start()
    q_cols = pl.ds(pl.multiple_of(cell * 256, 256), 256)
    q_rows = d_model // CHUNKS
    cp_wq = [
        pltpu.make_async_copy(
            wq_hbm.at[pl.ds(c * q_rows, q_rows), q_cols], wq.at[pl.ds(c * q_rows, q_rows), :], wq_sems.at[c]
        )
        for c in range(CHUNKS)
    ]
    kv_depth = d_model // SIDE
    kv_rows = pl.ds(pl.multiple_of(lx * kv_depth, kv_depth), kv_depth)
    kv_cols = pl.ds(pl.multiple_of(ly * head, head), head)
    cp_wk = pltpu.make_async_copy(wk_hbm.at[kv_rows, kv_cols], wk, sems.at[4])
    cp_wv = pltpu.make_async_copy(wv_hbm.at[kv_rows, kv_cols], wv, sems.at[5])
    cp_wk.start()
    cp_wv.start()
    for cp in cp_wq:
        cp.start()
    cp_k = pltpu.make_async_copy(k_hbm, kbuf, sems.at[6])
    cp_v = pltpu.make_async_copy(v_hbm, vbuf, sems.at[7])
    n_cols = wo.shape[1]
    o_cols = pl.ds(pl.multiple_of(cell * n_cols, n_cols), n_cols)
    cp_wo = pltpu.make_async_copy(wo_hbm.at[:, o_cols], wo, sems.at[8])

    barrier = pltpu.get_barrier_semaphore()
    for a, b in plane_steps:
        pl.semaphore_signal(barrier, inc=1, device_id={"sp": plane_peer(a, b), "tp": core})
    for step in (2, 1, 3):
        pl.semaphore_signal(barrier, inc=1, device_id={"sp": line_peer("z", step), "tp": core})
    pl.semaphore_signal(barrier, inc=1, device_id={"sp": me, "tp": 1 - core})

    cp_hid.wait()
    cp_gain.wait()
    resid = hid[...].astype(F32)
    scale = lax.rsqrt(jnp.mean(resid * resid, axis=-1, keepdims=True) + EPS)
    normed = (resid * scale * gain[...]).astype(BF16)

    rows[...] = normed.astype(F32)
    normed_kv = rows[:, kv_rows].astype(BF16)
    cp_wk.wait()
    cp_wv.wait()
    k_part = jnp.dot(normed_kv, wk[...], preferred_element_type=F32)
    v_part = jnp.dot(normed_kv, wv[...], preferred_element_type=F32)
    q_acc = [jnp.zeros((batch, 256), F32), jnp.zeros((batch, 256), F32)]
    for c in range(CHUNKS):
        if c == 2:
            cp_pos.wait()
            cp_freq.wait()
            row4 = lax.broadcasted_iota(jnp.int32, (batch, head), 0)
            lane4 = lax.broadcasted_iota(jnp.int32, (batch, head), 1)
            pos_rows = jnp.zeros((batch, head), jnp.int32)
            for b in range(batch):
                pos_rows = jnp.where(row4 == b, pos[b], pos_rows)
            angles = pos_rows.astype(F32) * freq[...]
            cosine = jnp.cos(angles)
            sine = jnp.sin(angles)
            sine = jnp.where(lane4 < head // 2, -sine, sine)
        cp_wq[c].wait()
        for u in range(2):
            lo, hi = c * q_rows + u * q_rows // 2, c * q_rows + (u + 1) * q_rows // 2
            q_acc[u] += jnp.dot(normed[:, lo:hi], wq[lo:hi, :], preferred_element_type=F32)
    cp_k.start()
    cp_v.start()

    q_acc = q_acc[0] + q_acc[1]

    def rotate(u):
        return u * cosine + pltpu.roll(u, head // 2, axis=1) * sine

    q_lo = rotate(q_acc[:, :head]).astype(BF16).astype(F32)
    q_hi = rotate(q_acc[:, head:]).astype(BF16).astype(F32)
    mine = pl.ds(pl.multiple_of(cell * 16, 16), 16)
    gathered[mine, :] = jnp.concatenate([q_lo, q_hi, k_part, v_part], axis=0)

    pl.semaphore_wait(barrier, PLANE - 1 + SIDE - 1 + 1)
    for a, b in plane_steps:
        pltpu.make_async_remote_copy(
            src_ref=gathered.at[mine], dst_ref=gathered.at[mine], send_sem=qsend, recv_sem=qrecv,
            device_id={"sp": plane_peer(a, b), "tp": core},
        ).start()
    cp_wo.start()
    cp_k.wait()
    for b in range(batch):
        kturn[b] = kbuf[b].T
    sum_bytes(gathered.at[pl.ds(0, 16 * (PLANE - 1))], qrecv)

    cos_all = jnp.concatenate([cosine] * 4, axis=0)
    sin_all = jnp.concatenate([sine] * 4, axis=0)
    k_sum, v_sum = [], []
    for j in range(4):
        k_sum.append(sum(gathered[(4 * j + i) * 16 + 8:(4 * j + i) * 16 + 12, :] for i in range(4)))
        v_sum.append(sum(gathered[(4 * j + i) * 16 + 12:(4 * j + i) * 16 + 16, :] for i in range(4)))
    k_all = jnp.concatenate(k_sum, axis=0)
    v_all = jnp.concatenate(v_sum, axis=0)
    k_all = k_all * cos_all + pltpu.roll(k_all, head // 2, axis=1) * sin_all
    fresh[0:16, :] = k_all.astype(BF16).astype(F32)
    fresh[16:32, :] = v_all.astype(BF16).astype(F32)

    cols = seq_local * 4
    tiles = cols // 128
    lane = lax.broadcasted_iota(jnp.int32, (32, 128), 1)
    row_head = (lax.broadcasted_iota(jnp.int32, (32, 128), 0) & 15) >> 2
    column = jnp.where((lane & 3) == row_head, lane, 1 << 30)
    new_row = (lax.broadcasted_iota(jnp.int32, (32, 16), 0) & 15) >> 2
    new_lane = lax.broadcasted_iota(jnp.int32, (32, 16), 1)
    new_head = new_row == new_lane
    to_log2 = head ** -0.5 * 1.4426950408889634
    base = me * seq_local
    pad = jnp.zeros((12, head), F32)
    dims_last = (((1,), (1,)), ((), ()))
    cp_v.wait()
    acc_rows, m_rows, l_rows = [], [], []
    for b in range(batch):
        k_b = jnp.concatenate([fresh[pl.ds(b, 4, stride=4), :], pad], axis=0).astype(BF16)
        v_b = jnp.concatenate([fresh[pl.ds(16 + b, 4, stride=4), :], pad], axis=0).astype(BF16)
        q_b = jnp.concatenate(
            [gathered[pl.ds(b, 16, stride=16), :], gathered[pl.ds(4 + b, 16, stride=16), :]], axis=0
        ).astype(BF16)
        limit = (pos[b] - base) * 4
        offset = new_lane * 0 + limit
        valid_new = jnp.logical_and(new_head, jnp.logical_and(offset >= 0, offset < cols))
        s_halves = [
            jnp.dot(q_b, kturn[b, :, u * cols // 2:(u + 1) * cols // 2], preferred_element_type=F32) for u in range(2)
        ]
        s_new = lax.dot_general(q_b, k_b, dims_last, preferred_element_type=F32)
        s_new = jnp.where(valid_new, s_new, NEG_BIG)
        s = []
        for i in range(tiles):
            u, j = divmod(i, tiles // 2)
            s.append(jnp.where(column < limit - 128 * i, s_halves[u][:, 128 * j:128 * (j + 1)], NEG_BIG))
        top = s
        while len(top) > 1:
            top = [jnp.maximum(top[i], top[i + 1]) for i in range(0, len(top), 2)]
        m = jnp.maximum(jnp.max(top[0], axis=-1, keepdims=True), jnp.max(s_new, axis=-1, keepdims=True))
        shift = jnp.where(m == NEG_BIG, 0.0, m)
        p = [jnp.exp2((si - shift) * to_log2) for si in s]
        p_new = jnp.exp2((s_new - shift) * to_log2)
        total = p
        while len(total) > 1:
            total = [total[i] + total[i + 1] for i in range(0, len(total), 2)]
        l_rows.append(jnp.sum(total[0], axis=-1, keepdims=True) + jnp.sum(p_new, axis=-1, keepdims=True))
        m_rows.append(m)
        half_tiles = tiles // 2
        pv = [
            jnp.dot(
                jnp.concatenate([pi.astype(BF16) for pi in p[u * half_tiles:(u + 1) * half_tiles]], axis=1),
                vbuf[b, u * cols // 2:(u + 1) * cols // 2, :],
                preferred_element_type=F32,
            )
            for u in range(2)
        ]
        acc_rows.append(pv[0] + pv[1] + jnp.dot(p_new.astype(BF16), v_b, preferred_element_type=F32))
    acc_t = jnp.concatenate(acc_rows, axis=0).T
    m_col = jnp.concatenate(m_rows, axis=0)
    l_col = jnp.concatenate(l_rows, axis=0)
    stat_lane = lax.broadcasted_iota(jnp.int32, (128, 128), 1)
    stat_t = jnp.where(stat_lane == 0, m_col, l_col).T[0:8]

    parts = (x0, x1, x2, x3, x4, x5, x6, x7, x8)

    def send_part(p, t):
        axis = AXES[(PARTS[p][0] + t) % 3]
        slot = parts[p].at[t, line[axis]]
        for step in (2, 1, 3):
            pltpu.make_async_remote_copy(
                src_ref=slot, dst_ref=slot, send_sem=part_send.at[p, t], recv_sem=part_recv.at[p, t],
                device_id={"sp": line_peer(axis, step), "tp": core},
            ).start()

    for p, (order, dims, has_stats) in enumerate(PARTS):
        slot = line[AXES[order]]
        parts[p][0, slot, 0:dims, :] = acc_t[STARTS[p]:STARTS[p] + dims]
        if has_stats:
            parts[p][0, slot, dims:dims + 8, :] = stat_t
        send_part(p, 0)

    tile_pos = lax.broadcasted_iota(jnp.int32, (16, head), 0) >> 2
    block = 256
    for buf, first in ((kbuf, 0), (vbuf, 16)):
        for b in range(batch):
            new4 = fresh[pl.ds(first + b, 4, stride=4), :]
            new16 = jnp.concatenate([new4] * 4, axis=0).astype(BF16)
            spot = pos[b] - base

            def patch(i, carry, buf=buf, b=b, new16=new16, spot=spot):
                for j in range(block // 16):
                    at = pl.ds(pl.multiple_of(i * block + j * 16, 16), 16)
                    hit = tile_pos == spot - i * (block // 4) - 4 * j
                    buf[b, at, :] = jnp.where(hit, new16, buf[b, at, :])
                return carry

            lax.fori_loop(0, cols // block, patch, 0)

    o_parts = []
    row8 = lax.broadcasted_iota(jnp.int32, (8, 128), 0)
    factors = {}
    for t in range(3):
        for p, (order, dims, has_stats) in enumerate(PARTS):
            ref = parts[p]
            sum_bytes(ref.at[t, pl.ds(0, SIDE - 1)], part_recv.at[p, t])
            if has_stats:
                stats = [ref[t, i, dims:dims + 8, :] for i in range(SIDE)]
                ms = [st[0:1] for st in stats]
                top = jnp.maximum(jnp.maximum(ms[0], ms[1]), jnp.maximum(ms[2], ms[3]))
                fac = [jnp.exp2((mi - top) * to_log2) for mi in ms]
                total = sum(stats[i][1:2] * fac[i] for i in range(SIDE))
                factors[order] = (fac, total)
            fac, total = factors[order]
            acc = sum(ref[t, i, 0:dims, :] * fac[i] for i in range(SIDE))
            if t < 2:
                slot = line[AXES[(order + t + 1) % 3]]
                ref[t + 1, slot, 0:dims, :] = acc
                if has_stats:
                    ref[t + 1, slot, dims:dims + 8, :] = jnp.where(row8 == 0, top, total)
                send_part(p, t + 1)
            else:
                o_parts.append(acc / total)
    orow[...] = jnp.concatenate(o_parts, axis=0).T

    attn = jnp.concatenate(
        [orow[pl.ds(h // 2 + 16 * (h % 2), batch, stride=32), :] for h in range(32)], axis=1
    ).astype(BF16)
    cp_wo.wait()
    o_rows = wo.shape[0] // CHUNKS
    half = n_cols // HALVES
    cp_tp = []
    for u in range(HALVES):
        y = [jnp.zeros((batch, half), F32), jnp.zeros((batch, half), F32)]
        for c in range(CHUNKS):
            y[c % 2] += jnp.dot(
                attn[:, c * o_rows:(c + 1) * o_rows],
                wo[c * o_rows:(c + 1) * o_rows, u * half:(u + 1) * half],
                preferred_element_type=F32,
            )
        ypart[u] = y[0] + y[1]
        cp_tp.append(
            pltpu.make_async_remote_copy(
                src_ref=ypart.at[u], dst_ref=ypeer.at[u], send_sem=tpsend.at[u], recv_sem=tprecv.at[u],
                device_id={"sp": me, "tp": 1 - core},
            )
        )
        cp_tp[u].start()
    for u in range(HALVES):
        cp_tp[u].wait_recv()
        yall[u, cell] = ypart[u] + ypeer[u]
        for a, b in plane_steps:
            pltpu.make_async_remote_copy(
                src_ref=yall.at[u, cell], dst_ref=yall.at[u, cell], send_sem=ysend.at[u], recv_sem=yrecv.at[u],
                device_id={"sp": plane_peer(a, b), "tp": core},
            ).start()

    sum_bytes(gathered.at[pl.ds(0, 16 * (PLANE - 1))], qsend)
    for t in range(3):
        for p in range(len(PARTS)):
            sum_bytes(parts[p].at[t, pl.ds(0, SIDE - 1)], part_send.at[p, t])
    for u in range(HALVES):
        cp_tp[u].wait_send()

    for u in range(HALVES):
        sum_bytes(yall.at[u, pl.ds(0, PLANE - 1)], yrecv.at[u])
        for i in range(PLANE):
            lo = i * n_cols + u * half
            out_ref[:, lo:lo + half] = (hid[:, lo:lo + half].astype(F32) + yall[u, i]).astype(BF16)
    for u in range(HALVES):
        sum_bytes(yall.at[u, pl.ds(0, PLANE - 1)], ysend.at[u])


def store_kernel(y_ref, k_ref, v_ref, out_ref, ko_ref, vo_ref, sems):
    copies = []
    for b in range(k_ref.shape[0]):
        copies.append(pltpu.make_async_copy(k_ref.at[b], ko_ref.at[b], sems.at[2 * b]))
        copies.append(pltpu.make_async_copy(v_ref.at[b], vo_ref.at[b], sems.at[2 * b + 1]))
    copies.append(pltpu.make_async_copy(y_ref, out_ref, sems.at[2 * k_ref.shape[0]]))
    for cp in copies:
        cp.start()
    for cp in copies:
        cp.wait()


def solution(mesh):
    def local_step(hidden, norm_gain, w_query, w_key, w_value, w_out, k_cache, v_cache, positions):
        batch, seq_local, kv_local, head = k_cache.shape
        d_model = hidden.shape[1]
        n_cols = w_out.shape[1] // PLANE
        half = np.arange(head // 2, dtype=np.float32) * np.float32(2.0) / np.float32(head)
        inv = (np.float32(1.0) / np.power(np.float32(ROPE_BASE), half)).astype(np.float32)
        freq = jnp.asarray(np.concatenate([inv, inv])[None, :])
        flat = (batch, seq_local * kv_local, head)
        hbm = pl.BlockSpec(memory_space=pltpu.HBM)
        vmem = pl.BlockSpec(memory_space=pltpu.VMEM)
        dma = pltpu.SemaphoreType.DMA
        y, k_next, v_next = pl.pallas_call(
            attention_kernel,
            out_shape=[
                jax.ShapeDtypeStruct(hidden.shape, BF16),
                jax.ShapeDtypeStruct(flat, BF16),
                jax.ShapeDtypeStruct(flat, BF16),
            ],
            in_specs=[hbm] * 10,
            out_specs=[vmem] * 3,
            scratch_shapes=[
                pltpu.VMEM(hidden.shape, BF16),
                pltpu.VMEM((1, d_model), F32),
                pltpu.VMEM((1, head), F32),
                pltpu.VMEM((d_model, 256), BF16),
                pltpu.VMEM((d_model // SIDE, head), BF16),
                pltpu.VMEM((d_model // SIDE, head), BF16),
                pltpu.VMEM((w_out.shape[0], n_cols), BF16),
                pltpu.VMEM((batch, head, seq_local * kv_local), BF16),
                pltpu.VMEM((PLANE * 16, head), F32),
                pltpu.VMEM((32, head), F32),
                pltpu.VMEM((batch, d_model), F32),
                *[pltpu.VMEM((3, SIDE, d + 8 * stats, 128), F32) for _, d, stats in PARTS],
                pltpu.VMEM((128, 128), F32),
                pltpu.VMEM((HALVES, batch, n_cols // HALVES), F32),
                pltpu.VMEM((HALVES, batch, n_cols // HALVES), F32),
                pltpu.VMEM((HALVES, PLANE, batch, n_cols // HALVES), F32),
                pltpu.SMEM((batch,), jnp.int32),
                dma((9,)),
                dma((CHUNKS,)),
                dma((len(PARTS), 3)),
                dma((len(PARTS), 3)),
                dma, dma,
                *[dma((HALVES,))] * 4,
            ],
            compiler_params=pltpu.CompilerParams(
                collective_id=0, has_side_effects=True, vmem_limit_bytes=30 << 20
            ),
            cost_estimate=pl.CostEstimate(flops=20_000_000_000, bytes_accessed=20_000_000, transcendentals=0),
            name="attention_step",
        )(
            *[
                pltpu.with_memory_space_constraint(a, pltpu.HBM)
                for a in (
                    hidden, norm_gain.reshape(1, d_model), freq, positions, w_query, w_key, w_value, w_out,
                    k_cache.reshape(flat), v_cache.reshape(flat),
                )
            ]
        )
        any_space = pl.BlockSpec(memory_space=pl.ANY)
        y, k_next, v_next = pl.pallas_call(
            store_kernel,
            out_shape=[
                jax.ShapeDtypeStruct(hidden.shape, BF16),
                jax.ShapeDtypeStruct(flat, BF16),
                jax.ShapeDtypeStruct(flat, BF16),
            ],
            in_specs=[vmem] * 3,
            out_specs=[any_space] * 3,
            scratch_shapes=[dma((2 * batch + 1,))],
            compiler_params=pltpu.CompilerParams(vmem_limit_bytes=16 << 20),
            cost_estimate=pl.CostEstimate(flops=1_000_000, bytes_accessed=8_000_000, transcendentals=0),
            name="cache_store",
        )(y, k_next, v_next)
        return y, k_next.reshape(k_cache.shape), v_next.reshape(v_cache.shape)

    cache_spec = P("dp", "sp", "tp", None)
    specs_in = (P("dp", None), P(None), P(None, "tp"), P(None, "tp"), P(None, "tp"), P("tp", None), cache_spec, cache_spec, P("dp"))
    specs_out = (P("dp", None), cache_spec, cache_spec)
    return jax.shard_map(local_step, mesh=mesh, in_specs=specs_in, out_specs=specs_out, check_vma=False)
```

```python
import jax
import jax.numpy as jnp
import numpy as np
from jax import lax
from jax.experimental import pallas as pl
from jax.experimental.pallas import tpu as pltpu
from jax.sharding import PartitionSpec as P

ROPE_BASE = 1000000.0
EPS = 1e-5
NEG_BIG = -3.0e38
SIDE = 4
PLANE = SIDE * SIDE
AXES = ("x", "y", "z")
PARTS = (
    (0, 16, True), (1, 16, True), (2, 16, True),
    (0, 16, False), (1, 16, False), (2, 16, False),
    (0, 16, False), (1, 8, False), (2, 8, False),
)
STARTS = tuple(sum(d for _, d, _ in PARTS[:i]) for i in range(len(PARTS)))
HALVES = 2
CHUNKS = 8
BF16 = jnp.bfloat16
F32 = jnp.float32


def sum_bytes(ref, sem):
    pltpu.make_async_copy(ref, ref, sem).wait()


def attention_kernel(
    hidden_hbm, gain_hbm, freq_hbm, pos_hbm, wq_hbm, wk_hbm, wv_hbm, wo_hbm, k_hbm, v_hbm,
    out_ref, kbuf, vbuf,
    hid, gain, freq, wq, wk, wv, wo, kturn, gathered, fresh, rows, x0, x1, x2, x3, x4, x5, x6, x7, x8, orow, stat, orow2,
    ypart, ypeer, yall, pos, sems, wq_sems, part_send, part_recv, qsend, qrecv, tpsend, tprecv, ysend, yrecv,
):
    batch, d_model = hid.shape
    head = 128
    seq_local = kbuf.shape[1] // 4
    me = lax.axis_index("sp")
    core = lax.axis_index("tp")
    lx = lax.rem(me, SIDE)
    ly = lax.rem(me // SIDE, SIDE)
    lz = me // PLANE
    cell = lax.rem(me, PLANE)
    line = {"x": lx, "y": ly, "z": lz}
    stride = {"x": 1, "y": SIDE, "z": PLANE}

    def line_peer(axis, step):
        here = line[axis]
        return me + (lax.rem(here + step, SIDE) - here) * stride[axis]

    def plane_peer(step_y, step_x):
        return lz * PLANE + lax.rem(ly + step_y, SIDE) * SIDE + lax.rem(lx + step_x, SIDE)

    plane_steps = sorted(
        [(a, b) for a in range(SIDE) for b in range(SIDE) if (a, b) != (0, 0)],
        key=lambda s: -(min(s[0], SIDE - s[0]) + min(s[1], SIDE - s[1])),
    )

    cp_hid = pltpu.make_async_copy(hidden_hbm, hid, sems.at[0])
    cp_gain = pltpu.make_async_copy(gain_hbm, gain, sems.at[1])
    cp_pos = pltpu.make_async_copy(pos_hbm, pos, sems.at[2])
    cp_freq = pltpu.make_async_copy(freq_hbm, freq, sems.at[3])
    for cp in (cp_hid, cp_gain, cp_pos, cp_freq):
        cp.start()
    q_cols = pl.ds(pl.multiple_of(cell * 256, 256), 256)
    q_rows = d_model // CHUNKS

    def copy_wq(c):
        here = pl.ds(pl.multiple_of(c * q_rows, q_rows), q_rows)
        return pltpu.make_async_copy(wq_hbm.at[here, q_cols], wq.at[here, :], wq_sems.at[c])

    kv_depth = d_model // SIDE
    kv_rows = pl.ds(pl.multiple_of(lx * kv_depth, kv_depth), kv_depth)
    kv_cols = pl.ds(pl.multiple_of(ly * head, head), head)
    cp_wk = pltpu.make_async_copy(wk_hbm.at[kv_rows, kv_cols], wk, sems.at[4])
    cp_wv = pltpu.make_async_copy(wv_hbm.at[kv_rows, kv_cols], wv, sems.at[5])
    cp_wk.start()
    cp_wv.start()
    for c in range(CHUNKS):
        copy_wq(c).start()
    cp_k = pltpu.make_async_copy(k_hbm, kbuf, sems.at[6])
    cp_v = pltpu.make_async_copy(v_hbm, vbuf, sems.at[7])
    n_cols = wo.shape[1]
    o_cols = pl.ds(pl.multiple_of(cell * n_cols, n_cols), n_cols)
    cp_wo = pltpu.make_async_copy(wo_hbm.at[:, o_cols], wo, sems.at[8])

    barrier = pltpu.get_barrier_semaphore()
    for a, b in plane_steps:
        pl.semaphore_signal(barrier, inc=1, device_id={"sp": plane_peer(a, b), "tp": core})
    for step in (2, 1, 3):
        pl.semaphore_signal(barrier, inc=1, device_id={"sp": line_peer("z", step), "tp": core})
    pl.semaphore_signal(barrier, inc=1, device_id={"sp": me, "tp": 1 - core})

    cp_hid.wait()
    cp_gain.wait()
    resid = hid[...].astype(F32)
    scale = lax.rsqrt(jnp.mean(resid * resid, axis=-1, keepdims=True) + EPS)
    normed = (resid * scale * gain[...]).astype(BF16)

    rows[...] = normed.astype(F32)
    normed_kv = rows[:, kv_rows].astype(BF16)
    cp_wk.wait()
    cp_wv.wait()
    k_part = jnp.dot(normed_kv, wk[...], preferred_element_type=F32)
    v_part = jnp.dot(normed_kv, wv[...], preferred_element_type=F32)
    cp_pos.wait()
    cp_freq.wait()
    row4 = lax.broadcasted_iota(jnp.int32, (batch, head), 0)
    lane4 = lax.broadcasted_iota(jnp.int32, (batch, head), 1)
    pos_rows = jnp.zeros((batch, head), jnp.int32)
    for b in range(batch):
        pos_rows = jnp.where(row4 == b, pos[b], pos_rows)
    angles = pos_rows.astype(F32) * freq[...]
    cosine = jnp.cos(angles)
    sine = jnp.sin(angles)
    sine = jnp.where(lane4 < head // 2, -sine, sine)

    def project(c, acc):
        at = pl.multiple_of(c * q_rows, q_rows)
        copy_wq(c).wait()
        acc = list(acc)
        for u in range(2):
            here = pl.ds(at + u * (q_rows // 2), q_rows // 2)
            acc[u] += jnp.dot(rows[:, here].astype(BF16), wq[here, :], preferred_element_type=F32)
        return tuple(acc)

    q_acc = lax.fori_loop(0, CHUNKS, project, (jnp.zeros((batch, 256), F32), jnp.zeros((batch, 256), F32)))
    cp_k.start()
    cp_v.start()

    q_acc = q_acc[0] + q_acc[1]

    def rotate(u):
        return u * cosine + pltpu.roll(u, head // 2, axis=1) * sine

    q_lo = rotate(q_acc[:, :head]).astype(BF16).astype(F32)
    q_hi = rotate(q_acc[:, head:]).astype(BF16).astype(F32)
    mine = pl.ds(pl.multiple_of(cell * 16, 16), 16)
    gathered[mine, :] = jnp.concatenate([q_lo, q_hi, k_part, v_part], axis=0)

    pl.semaphore_wait(barrier, PLANE - 1 + SIDE - 1 + 1)
    for a, b in plane_steps:
        pltpu.make_async_remote_copy(
            src_ref=gathered.at[mine], dst_ref=gathered.at[mine], send_sem=qsend, recv_sem=qrecv,
            device_id={"sp": plane_peer(a, b), "tp": core},
        ).start()
    cp_wo.start()
    cp_k.wait()
    for b in range(batch):
        kturn[b] = kbuf[b].T
    sum_bytes(gathered.at[pl.ds(0, 16 * (PLANE - 1))], qrecv)

    cos_all = jnp.concatenate([cosine] * 4, axis=0)
    sin_all = jnp.concatenate([sine] * 4, axis=0)
    k_sum, v_sum = [], []
    for j in range(4):
        k_sum.append(sum(gathered[(4 * j + i) * 16 + 8:(4 * j + i) * 16 + 12, :] for i in range(4)))
        v_sum.append(sum(gathered[(4 * j + i) * 16 + 12:(4 * j + i) * 16 + 16, :] for i in range(4)))
    k_all = jnp.concatenate(k_sum, axis=0)
    v_all = jnp.concatenate(v_sum, axis=0)
    k_all = k_all * cos_all + pltpu.roll(k_all, head // 2, axis=1) * sin_all
    fresh[0:16, :] = k_all.astype(BF16).astype(F32)
    fresh[16:32, :] = v_all.astype(BF16).astype(F32)

    cols = seq_local * 4
    tiles = cols // 128
    lane = lax.broadcasted_iota(jnp.int32, (32, 128), 1)
    row_head = (lax.broadcasted_iota(jnp.int32, (32, 128), 0) & 15) >> 2
    column = jnp.where((lane & 3) == row_head, lane, 1 << 30)
    new_row = (lax.broadcasted_iota(jnp.int32, (32, 16), 0) & 15) >> 2
    new_lane = lax.broadcasted_iota(jnp.int32, (32, 16), 1)
    new_head = new_row == new_lane
    to_log2 = head ** -0.5 * 1.4426950408889634
    base = me * seq_local
    pad = jnp.zeros((12, head), F32)
    dims_last = (((1,), (1,)), ((), ()))
    cp_v.wait()

    def attend(b):
        k_b = jnp.concatenate([fresh[pl.ds(b, 4, stride=4), :], pad], axis=0).astype(BF16)
        v_b = jnp.concatenate([fresh[pl.ds(16 + b, 4, stride=4), :], pad], axis=0).astype(BF16)
        q_b = jnp.concatenate(
            [gathered[pl.ds(b, 16, stride=16), :], gathered[pl.ds(4 + b, 16, stride=16), :]], axis=0
        ).astype(BF16)
        limit = (pos[b] - base) * 4
        offset = new_lane * 0 + limit
        valid_new = jnp.logical_and(new_head, jnp.logical_and(offset >= 0, offset < cols))
        s_halves = [
            jnp.dot(q_b, kturn[b, :, u * cols // 2:(u + 1) * cols // 2], preferred_element_type=F32) for u in range(2)
        ]
        s_new = lax.dot_general(q_b, k_b, dims_last, preferred_element_type=F32)
        s_new = jnp.where(valid_new, s_new, NEG_BIG)
        s = []
        for i in range(tiles):
            u, j = divmod(i, tiles // 2)
            s.append(jnp.where(column < limit - 128 * i, s_halves[u][:, 128 * j:128 * (j + 1)], NEG_BIG))
        top = s
        while len(top) > 1:
            top = [jnp.maximum(top[i], top[i + 1]) for i in range(0, len(top), 2)]
        m = jnp.maximum(jnp.max(top[0], axis=-1, keepdims=True), jnp.max(s_new, axis=-1, keepdims=True))
        shift = jnp.where(m == NEG_BIG, 0.0, m)
        p = [jnp.exp2((si - shift) * to_log2) for si in s]
        p_new = jnp.exp2((s_new - shift) * to_log2)
        total = p
        while len(total) > 1:
            total = [total[i] + total[i + 1] for i in range(0, len(total), 2)]
        l = jnp.sum(total[0], axis=-1, keepdims=True) + jnp.sum(p_new, axis=-1, keepdims=True)
        half_tiles = tiles // 2
        pv = [
            jnp.dot(
                jnp.concatenate([pi.astype(BF16) for pi in p[u * half_tiles:(u + 1) * half_tiles]], axis=1),
                vbuf[b, u * cols // 2:(u + 1) * cols // 2, :],
                preferred_element_type=F32,
            )
            for u in range(2)
        ]
        here = pl.ds(pl.multiple_of(b * 32, 32), 32)
        orow[here, :] = pv[0] + pv[1] + jnp.dot(p_new.astype(BF16), v_b, preferred_element_type=F32)
        stat[here, :] = jnp.where(lane == 0, m, l)

    def attend_some(g, carry):
        for i in range(4):
            attend(g * 4 + i)
        return carry

    lax.fori_loop(0, batch // 4, attend_some, 0)
    acc_t = orow[...].T
    stat_t = stat[...].T[0:8]

    parts = (x0, x1, x2, x3, x4, x5, x6, x7, x8)

    def send_part(p, t):
        axis = AXES[(PARTS[p][0] + t) % 3]
        slot = parts[p].at[t, line[axis]]
        for step in (2, 1, 3):
            pltpu.make_async_remote_copy(
                src_ref=slot, dst_ref=slot, send_sem=part_send.at[p, t], recv_sem=part_recv.at[p, t],
                device_id={"sp": line_peer(axis, step), "tp": core},
            ).start()

    for p, (order, dims, has_stats) in enumerate(PARTS):
        slot = line[AXES[order]]
        parts[p][0, slot, 0:dims, :] = acc_t[STARTS[p]:STARTS[p] + dims]
        if has_stats:
            parts[p][0, slot, dims:dims + 8, :] = stat_t
        send_part(p, 0)

    tile_pos = (lax.broadcasted_iota(jnp.int32, (16, head), 0) >> 2).astype(F32)
    block = 256

    def patch_cache(buf, first):
        for b in range(batch):
            new4 = fresh[pl.ds(first + b, 4, stride=4), :]
            new16 = jnp.concatenate([new4] * 4, axis=0).astype(BF16)
            spot = pos[b] - base

            def patch(i, carry, b=b, new16=new16, spot=spot):
                ahead = jnp.clip(spot - i * (block // 4), -1, block // 4).astype(F32)
                ahead = (ahead - tile_pos).astype(BF16)
                at = pl.ds(pl.multiple_of(i * block, block), block)
                old = buf[b, at, :]
                buf[b, at, :] = jnp.concatenate(
                    [jnp.where(ahead == 4 * j, new16, old[16 * j:16 * (j + 1)]) for j in range(block // 16)], axis=0
                )
                return carry

            lax.fori_loop(0, cols // block, patch, 0)

    patch_cache(vbuf, 16)
    patch_cache(kbuf, 0)

    o_parts = []
    row8 = lax.broadcasted_iota(jnp.int32, (8, 128), 0)
    factors = {}
    for t in range(3):
        for p, (order, dims, has_stats) in enumerate(PARTS):
            ref = parts[p]
            sum_bytes(ref.at[t, pl.ds(0, SIDE - 1)], part_recv.at[p, t])
            if has_stats:
                stats = [ref[t, i, dims:dims + 8, :] for i in range(SIDE)]
                ms = [st[0:1] for st in stats]
                top = jnp.maximum(jnp.maximum(ms[0], ms[1]), jnp.maximum(ms[2], ms[3]))
                fac = [jnp.exp2((mi - top) * to_log2) for mi in ms]
                total = sum(stats[i][1:2] * fac[i] for i in range(SIDE))
                factors[order] = (fac, total)
            fac, total = factors[order]
            acc = sum(ref[t, i, 0:dims, :] * fac[i] for i in range(SIDE))
            if t < 2:
                slot = line[AXES[(order + t + 1) % 3]]
                ref[t + 1, slot, 0:dims, :] = acc
                if has_stats:
                    ref[t + 1, slot, dims:dims + 8, :] = jnp.where(row8 == 0, top, total)
                send_part(p, t + 1)
            else:
                o_parts.append(acc / total)
    orow[...] = jnp.concatenate(o_parts, axis=0).T

    attn = jnp.concatenate(
        [orow[pl.ds(h // 2 + 16 * (h % 2), batch, stride=32), :] for h in range(32)], axis=1
    ).astype(BF16)
    cp_wo.wait()
    o_rows = wo.shape[0] // CHUNKS
    half = n_cols // HALVES

    def copy_tp(u):
        return pltpu.make_async_remote_copy(
            src_ref=ypart.at[u], dst_ref=ypeer.at[u], send_sem=tpsend.at[u], recv_sem=tprecv.at[u],
            device_id={"sp": me, "tp": 1 - core},
        )

    def project_out(u, carry):
        here = pl.ds(pl.multiple_of(u * half, half), half)
        y = [jnp.zeros((batch, half), F32), jnp.zeros((batch, half), F32)]
        for c in range(CHUNKS):
            y[c % 2] += jnp.dot(
                orow2[:, c * o_rows:(c + 1) * o_rows],
                wo[c * o_rows:(c + 1) * o_rows, here],
                preferred_element_type=F32,
            )
        ypart[u] = y[0] + y[1]
        copy_tp(u).start()
        return carry

    orow2[...] = attn
    lax.fori_loop(0, HALVES, project_out, 0)
    cp_tp = [copy_tp(u) for u in range(HALVES)]
    for u in range(HALVES):
        cp_tp[u].wait_recv()
        yall[u, cell] = ypart[u] + ypeer[u]
        for a, b in plane_steps:
            pltpu.make_async_remote_copy(
                src_ref=yall.at[u, cell], dst_ref=yall.at[u, cell], send_sem=ysend.at[u], recv_sem=yrecv.at[u],
                device_id={"sp": plane_peer(a, b), "tp": core},
            ).start()

    sum_bytes(gathered.at[pl.ds(0, 16 * (PLANE - 1))], qsend)
    for t in range(3):
        for p in range(len(PARTS)):
            sum_bytes(parts[p].at[t, pl.ds(0, SIDE - 1)], part_send.at[p, t])
    for u in range(HALVES):
        cp_tp[u].wait_send()

    for u in range(HALVES):
        sum_bytes(yall.at[u, pl.ds(0, PLANE - 1)], yrecv.at[u])
        for i in range(PLANE):
            lo = i * n_cols + u * half
            out_ref[:, lo:lo + half] = (hid[:, lo:lo + half].astype(F32) + yall[u, i]).astype(BF16)
    for u in range(HALVES):
        sum_bytes(yall.at[u, pl.ds(0, PLANE - 1)], ysend.at[u])


def store_kernel(y_ref, k_ref, v_ref, out_ref, ko_ref, vo_ref, sems):
    copies = []
    for b in range(k_ref.shape[0]):
        copies.append(pltpu.make_async_copy(k_ref.at[b], ko_ref.at[b], sems.at[2 * b]))
        copies.append(pltpu.make_async_copy(v_ref.at[b], vo_ref.at[b], sems.at[2 * b + 1]))
    copies.append(pltpu.make_async_copy(y_ref, out_ref, sems.at[2 * k_ref.shape[0]]))
    for cp in copies:
        cp.start()
    for cp in copies:
        cp.wait()


def solution(mesh):
    def local_step(hidden, norm_gain, w_query, w_key, w_value, w_out, k_cache, v_cache, positions):
        batch, seq_local, kv_local, head = k_cache.shape
        d_model = hidden.shape[1]
        n_cols = w_out.shape[1] // PLANE
        half = np.arange(head // 2, dtype=np.float32) * np.float32(2.0) / np.float32(head)
        inv = (np.float32(1.0) / np.power(np.float32(ROPE_BASE), half)).astype(np.float32)
        freq = jnp.asarray(np.concatenate([inv, inv])[None, :])
        flat = (batch, seq_local * kv_local, head)
        hbm = pl.BlockSpec(memory_space=pltpu.HBM)
        vmem = pl.BlockSpec(memory_space=pltpu.VMEM)
        dma = pltpu.SemaphoreType.DMA
        y, k_next, v_next = pl.pallas_call(
            attention_kernel,
            out_shape=[
                jax.ShapeDtypeStruct(hidden.shape, BF16),
                jax.ShapeDtypeStruct(flat, BF16),
                jax.ShapeDtypeStruct(flat, BF16),
            ],
            in_specs=[hbm] * 10,
            out_specs=[vmem] * 3,
            scratch_shapes=[
                pltpu.VMEM(hidden.shape, BF16),
                pltpu.VMEM((1, d_model), F32),
                pltpu.VMEM((1, head), F32),
                pltpu.VMEM((d_model, 256), BF16),
                pltpu.VMEM((d_model // SIDE, head), BF16),
                pltpu.VMEM((d_model // SIDE, head), BF16),
                pltpu.VMEM((w_out.shape[0], n_cols), BF16),
                pltpu.VMEM((batch, head, seq_local * kv_local), BF16),
                pltpu.VMEM((PLANE * 16, head), F32),
                pltpu.VMEM((32, head), F32),
                pltpu.VMEM((batch, d_model), F32),
                *[pltpu.VMEM((3, SIDE, d + 8 * stats, 128), F32) for _, d, stats in PARTS],
                pltpu.VMEM((128, 128), F32),
                pltpu.VMEM((128, 128), F32),
                pltpu.VMEM((batch, w_out.shape[0]), BF16),
                pltpu.VMEM((HALVES, batch, n_cols // HALVES), F32),
                pltpu.VMEM((HALVES, batch, n_cols // HALVES), F32),
                pltpu.VMEM((HALVES, PLANE, batch, n_cols // HALVES), F32),
                pltpu.SMEM((batch,), jnp.int32),
                dma((9,)),
                dma((CHUNKS,)),
                dma((len(PARTS), 3)),
                dma((len(PARTS), 3)),
                dma, dma,
                *[dma((HALVES,))] * 4,
            ],
            compiler_params=pltpu.CompilerParams(
                collective_id=0, has_side_effects=True, vmem_limit_bytes=30 << 20
            ),
            cost_estimate=pl.CostEstimate(flops=20_000_000_000, bytes_accessed=20_000_000, transcendentals=0),
            name="attention_step",
        )(
            *[
                pltpu.with_memory_space_constraint(a, pltpu.HBM)
                for a in (
                    hidden, norm_gain.reshape(1, d_model), freq, positions, w_query, w_key, w_value, w_out,
                    k_cache.reshape(flat), v_cache.reshape(flat),
                )
            ]
        )
        any_space = pl.BlockSpec(memory_space=pl.ANY)
        y, k_next, v_next = pl.pallas_call(
            store_kernel,
            out_shape=[
                jax.ShapeDtypeStruct(hidden.shape, BF16),
                jax.ShapeDtypeStruct(flat, BF16),
                jax.ShapeDtypeStruct(flat, BF16),
            ],
            in_specs=[vmem] * 3,
            out_specs=[any_space] * 3,
            scratch_shapes=[dma((2 * batch + 1,))],
            compiler_params=pltpu.CompilerParams(vmem_limit_bytes=16 << 20),
            cost_estimate=pl.CostEstimate(flops=1_000_000, bytes_accessed=8_000_000, transcendentals=0),
            name="cache_store",
        )(y, k_next, v_next)
        return y, k_next.reshape(k_cache.shape), v_next.reshape(v_cache.shape)

    cache_spec = P("dp", "sp", "tp", None)
    specs_in = (P("dp", None), P(None), P(None, "tp"), P(None, "tp"), P(None, "tp"), P("tp", None), cache_spec, cache_spec, P("dp"))
    specs_out = (P("dp", None), cache_spec, cache_spec)
    return jax.shard_map(local_step, mesh=mesh, in_specs=specs_in, out_specs=specs_out, check_vma=False)
```

```python
import jax
import jax.numpy as jnp
import numpy as np
from jax import lax
from jax.experimental import pallas as pl
from jax.experimental.pallas import tpu as pltpu
from jax.sharding import PartitionSpec as P

ROPE_BASE = 1000000.0
EPS = 1e-5
NEG_BIG = -3.0e38
SIDE = 4
PLANE = SIDE * SIDE
AXES = ("x", "y", "z")
PARTS = (
    (0, 16, True), (1, 16, True), (2, 16, True),
    (0, 16, False), (1, 16, False), (2, 16, False),
    (0, 16, False), (1, 8, False), (2, 8, False),
)
STARTS = tuple(sum(d for _, d, _ in PARTS[:i]) for i in range(len(PARTS)))
HALVES = 1
CHUNKS = 8
BF16 = jnp.bfloat16
F32 = jnp.float32


def sum_bytes(ref, sem):
    pltpu.make_async_copy(ref, ref, sem).wait()


def attention_kernel(
    hidden_hbm, gain_hbm, freq_hbm, pos_hbm, wq_hbm, wk_hbm, wv_hbm, wo_hbm, k_hbm, v_hbm,
    out_ref, kbuf, vbuf,
    hid, gain, freq, wq, wk, wv, wo, kturn, gathered, fresh, rows, x0, x1, x2, x3, x4, x5, x6, x7, x8, orow, stat,
    ypart, ypeer, yall, pos, sems, wq_sems, part_send, part_recv, qsend, qrecv, tpsend, tprecv, ysend, yrecv,
):
    batch, d_model = hid.shape
    head = 128
    seq_local = kbuf.shape[1] // 4
    me = lax.axis_index("sp")
    core = lax.axis_index("tp")
    lx = lax.rem(me, SIDE)
    ly = lax.rem(me // SIDE, SIDE)
    lz = me // PLANE
    cell = lax.rem(me, PLANE)
    line = {"x": lx, "y": ly, "z": lz}
    stride = {"x": 1, "y": SIDE, "z": PLANE}

    def line_peer(axis, step):
        here = line[axis]
        return me + (lax.rem(here + step, SIDE) - here) * stride[axis]

    def plane_peer(step_y, step_x):
        return lz * PLANE + lax.rem(ly + step_y, SIDE) * SIDE + lax.rem(lx + step_x, SIDE)

    plane_steps = sorted(
        [(a, b) for a in range(SIDE) for b in range(SIDE) if (a, b) != (0, 0)],
        key=lambda s: -(min(s[0], SIDE - s[0]) + min(s[1], SIDE - s[1])),
    )

    cp_hid = pltpu.make_async_copy(hidden_hbm, hid, sems.at[0])
    cp_gain = pltpu.make_async_copy(gain_hbm, gain, sems.at[1])
    cp_pos = pltpu.make_async_copy(pos_hbm, pos, sems.at[2])
    cp_freq = pltpu.make_async_copy(freq_hbm, freq, sems.at[3])
    for cp in (cp_hid, cp_gain, cp_pos, cp_freq):
        cp.start()
    q_cols = pl.ds(pl.multiple_of(cell * 256, 256), 256)
    q_rows = d_model // CHUNKS

    def copy_wq(c):
        here = pl.ds(pl.multiple_of(c * q_rows, q_rows), q_rows)
        return pltpu.make_async_copy(wq_hbm.at[here, q_cols], wq.at[here, :], wq_sems.at[c])

    kv_depth = d_model // SIDE
    kv_rows = pl.ds(pl.multiple_of(lx * kv_depth, kv_depth), kv_depth)
    kv_cols = pl.ds(pl.multiple_of(ly * head, head), head)
    cp_wk = pltpu.make_async_copy(wk_hbm.at[kv_rows, kv_cols], wk, sems.at[4])
    cp_wv = pltpu.make_async_copy(wv_hbm.at[kv_rows, kv_cols], wv, sems.at[5])
    cp_wk.start()
    cp_wv.start()
    for c in range(CHUNKS):
        copy_wq(c).start()
    cp_k = pltpu.make_async_copy(k_hbm, kbuf, sems.at[6])
    cp_v = pltpu.make_async_copy(v_hbm, vbuf, sems.at[7])
    n_cols = wo.shape[1]
    o_cols = pl.ds(pl.multiple_of(cell * n_cols, n_cols), n_cols)
    cp_wo = pltpu.make_async_copy(wo_hbm.at[:, o_cols], wo, sems.at[8])

    barrier = pltpu.get_barrier_semaphore()
    for a, b in plane_steps:
        pl.semaphore_signal(barrier, inc=1, device_id={"sp": plane_peer(a, b), "tp": core})
    for step in (2, 1, 3):
        pl.semaphore_signal(barrier, inc=1, device_id={"sp": line_peer("z", step), "tp": core})
    pl.semaphore_signal(barrier, inc=1, device_id={"sp": me, "tp": 1 - core})

    cp_hid.wait()
    cp_gain.wait()
    resid = hid[...].astype(F32)
    scale = lax.rsqrt(jnp.mean(resid * resid, axis=-1, keepdims=True) + EPS)
    normed = (resid * scale * gain[...]).astype(BF16)

    rows[...] = normed.astype(F32)
    normed_kv = rows[:, kv_rows].astype(BF16)
    cp_wk.wait()
    cp_wv.wait()
    k_part = jnp.dot(normed_kv, wk[...], preferred_element_type=F32)
    v_part = jnp.dot(normed_kv, wv[...], preferred_element_type=F32)
    cp_pos.wait()
    cp_freq.wait()
    row4 = lax.broadcasted_iota(jnp.int32, (batch, head), 0)
    lane4 = lax.broadcasted_iota(jnp.int32, (batch, head), 1)
    pos_rows = jnp.zeros((batch, head), jnp.int32)
    for b in range(batch):
        pos_rows = jnp.where(row4 == b, pos[b], pos_rows)
    angles = pos_rows.astype(F32) * freq[...]
    cosine = jnp.cos(angles)
    sine = jnp.sin(angles)
    sine = jnp.where(lane4 < head // 2, -sine, sine)

    def project(c, acc):
        at = pl.multiple_of(c * q_rows, q_rows)
        copy_wq(c).wait()
        acc = list(acc)
        for u in range(2):
            here = pl.ds(at + u * (q_rows // 2), q_rows // 2)
            acc[u] += jnp.dot(rows[:, here].astype(BF16), wq[here, :], preferred_element_type=F32)
        return tuple(acc)

    q_acc = lax.fori_loop(0, CHUNKS, project, (jnp.zeros((batch, 256), F32), jnp.zeros((batch, 256), F32)))
    cp_k.start()
    cp_v.start()

    q_acc = q_acc[0] + q_acc[1]

    def rotate(u):
        return u * cosine + pltpu.roll(u, head // 2, axis=1) * sine

    q_lo = rotate(q_acc[:, :head]).astype(BF16).astype(F32)
    q_hi = rotate(q_acc[:, head:]).astype(BF16).astype(F32)
    mine = pl.ds(pl.multiple_of(cell * 16, 16), 16)
    gathered[mine, :] = jnp.concatenate([q_lo, q_hi, k_part, v_part], axis=0)

    pl.semaphore_wait(barrier, PLANE - 1 + SIDE - 1 + 1)
    for a, b in plane_steps:
        pltpu.make_async_remote_copy(
            src_ref=gathered.at[mine], dst_ref=gathered.at[mine], send_sem=qsend, recv_sem=qrecv,
            device_id={"sp": plane_peer(a, b), "tp": core},
        ).start()
    cp_wo.start()
    cp_k.wait()
    for b in range(batch):
        kturn[b] = kbuf[b].T
    sum_bytes(gathered.at[pl.ds(0, 16 * (PLANE - 1))], qrecv)

    cos_all = jnp.concatenate([cosine] * 4, axis=0)
    sin_all = jnp.concatenate([sine] * 4, axis=0)
    k_sum, v_sum = [], []
    for j in range(4):
        k_sum.append(sum(gathered[(4 * j + i) * 16 + 8:(4 * j + i) * 16 + 12, :] for i in range(4)))
        v_sum.append(sum(gathered[(4 * j + i) * 16 + 12:(4 * j + i) * 16 + 16, :] for i in range(4)))
    k_all = jnp.concatenate(k_sum, axis=0)
    v_all = jnp.concatenate(v_sum, axis=0)
    k_all = k_all * cos_all + pltpu.roll(k_all, head // 2, axis=1) * sin_all
    fresh[0:16, :] = k_all.astype(BF16).astype(F32)
    fresh[16:32, :] = v_all.astype(BF16).astype(F32)

    cols = seq_local * 4
    tiles = cols // 128
    lane = lax.broadcasted_iota(jnp.int32, (32, 128), 1)
    row_head = (lax.broadcasted_iota(jnp.int32, (32, 128), 0) & 15) >> 2
    column = jnp.where((lane & 3) == row_head, lane, 1 << 30)
    new_row = (lax.broadcasted_iota(jnp.int32, (32, 16), 0) & 15) >> 2
    new_lane = lax.broadcasted_iota(jnp.int32, (32, 16), 1)
    new_head = new_row == new_lane
    to_log2 = head ** -0.5 * 1.4426950408889634
    base = me * seq_local
    pad = jnp.zeros((12, head), F32)
    dims_last = (((1,), (1,)), ((), ()))
    cp_v.wait()

    half_tiles = tiles // 2

    def scores(b):
        k_b = jnp.concatenate([fresh[pl.ds(b, 4, stride=4), :], pad], axis=0).astype(BF16)
        q_b = jnp.concatenate(
            [gathered[pl.ds(b, 16, stride=16), :], gathered[pl.ds(4 + b, 16, stride=16), :]], axis=0
        ).astype(BF16)
        limit = (pos[b] - base) * 4
        offset = new_lane * 0 + limit
        valid_new = jnp.logical_and(new_head, jnp.logical_and(offset >= 0, offset < cols))
        s_halves = [
            jnp.dot(q_b, kturn[b, :, u * cols // 2:(u + 1) * cols // 2], preferred_element_type=F32) for u in range(2)
        ]
        s_new = lax.dot_general(q_b, k_b, dims_last, preferred_element_type=F32)
        s_new = jnp.where(valid_new, s_new, NEG_BIG)
        s = []
        for i in range(tiles):
            u, j = divmod(i, half_tiles)
            s.append(jnp.where(column < limit - 128 * i, s_halves[u][:, 128 * j:128 * (j + 1)], NEG_BIG))
        return s, s_new

    def weights(b, s, s_new):
        top = s
        while len(top) > 1:
            top = [jnp.maximum(top[i], top[i + 1]) for i in range(0, len(top), 2)]
        m = jnp.maximum(jnp.max(top[0], axis=-1, keepdims=True), jnp.max(s_new, axis=-1, keepdims=True))
        shift = jnp.where(m == NEG_BIG, 0.0, m)
        p = [jnp.exp2((si - shift) * to_log2) for si in s]
        p_new = jnp.exp2((s_new - shift) * to_log2)
        total = p
        while len(total) > 1:
            total = [total[i] + total[i + 1] for i in range(0, len(total), 2)]
        l = jnp.sum(total[0], axis=-1, keepdims=True) + jnp.sum(p_new, axis=-1, keepdims=True)
        stat[32 * b:32 * (b + 1), :] = jnp.where(lane == 0, m, l)
        halves = [
            jnp.concatenate([pi.astype(BF16) for pi in p[u * half_tiles:(u + 1) * half_tiles]], axis=1) for u in range(2)
        ]
        return halves, p_new.astype(BF16)

    def values(b, halves, p_new):
        v_b = jnp.concatenate([fresh[pl.ds(16 + b, 4, stride=4), :], pad], axis=0).astype(BF16)
        pv = [
            jnp.dot(halves[u], vbuf[b, u * cols // 2:(u + 1) * cols // 2, :], preferred_element_type=F32) for u in range(2)
        ]
        orow[32 * b:32 * (b + 1), :] = pv[0] + pv[1] + jnp.dot(p_new, v_b, preferred_element_type=F32)

    ready = scores(0)
    for b in range(batch):
        coming = scores(b + 1) if b + 1 < batch else None
        values(b, *weights(b, *ready))
        ready = coming
    acc_t = orow[...].T
    stat_t = stat[...].T[0:8]

    parts = (x0, x1, x2, x3, x4, x5, x6, x7, x8)

    def send_part(p, t):
        axis = AXES[(PARTS[p][0] + t) % 3]
        slot = parts[p].at[t, line[axis]]
        for step in (2, 1, 3):
            pltpu.make_async_remote_copy(
                src_ref=slot, dst_ref=slot, send_sem=part_send.at[p, t], recv_sem=part_recv.at[p, t],
                device_id={"sp": line_peer(axis, step), "tp": core},
            ).start()

    for p, (order, dims, has_stats) in enumerate(PARTS):
        slot = line[AXES[order]]
        parts[p][0, slot, 0:dims, :] = acc_t[STARTS[p]:STARTS[p] + dims]
        if has_stats:
            parts[p][0, slot, dims:dims + 8, :] = stat_t
        send_part(p, 0)

    tile_pos = (lax.broadcasted_iota(jnp.int32, (16, head), 0) >> 2).astype(F32)
    block = 256

    def patch_cache(buf, first):
        for b in range(batch):
            new4 = fresh[pl.ds(first + b, 4, stride=4), :]
            new16 = jnp.concatenate([new4] * 4, axis=0).astype(BF16)
            spot = pos[b] - base

            def patch(i, carry, b=b, new16=new16, spot=spot):
                ahead = jnp.clip(spot - i * (block // 4), -1, block // 4).astype(F32)
                ahead = (ahead - tile_pos).astype(BF16)
                at = pl.ds(pl.multiple_of(i * block, block), block)
                old = buf[b, at, :]
                buf[b, at, :] = jnp.concatenate(
                    [jnp.where(ahead == 4 * j, new16, old[16 * j:16 * (j + 1)]) for j in range(block // 16)], axis=0
                )
                return carry

            lax.fori_loop(0, cols // block, patch, 0)

    patch_cache(vbuf, 16)
    patch_cache(kbuf, 0)

    o_parts = []
    row8 = lax.broadcasted_iota(jnp.int32, (8, 128), 0)
    factors = {}
    for t in range(3):
        for p, (order, dims, has_stats) in enumerate(PARTS):
            ref = parts[p]
            sum_bytes(ref.at[t, pl.ds(0, SIDE - 1)], part_recv.at[p, t])
            if has_stats:
                stats = [ref[t, i, dims:dims + 8, :] for i in range(SIDE)]
                ms = [st[0:1] for st in stats]
                top = jnp.maximum(jnp.maximum(ms[0], ms[1]), jnp.maximum(ms[2], ms[3]))
                fac = [jnp.exp2((mi - top) * to_log2) for mi in ms]
                total = sum(stats[i][1:2] * fac[i] for i in range(SIDE))
                factors[order] = (fac, total)
            fac, total = factors[order]
            acc = sum(ref[t, i, 0:dims, :] * fac[i] for i in range(SIDE))
            if t < 2:
                slot = line[AXES[(order + t + 1) % 3]]
                ref[t + 1, slot, 0:dims, :] = acc
                if has_stats:
                    ref[t + 1, slot, dims:dims + 8, :] = jnp.where(row8 == 0, top, total)
                send_part(p, t + 1)
            else:
                o_parts.append(acc / total)
    orow[...] = jnp.concatenate(o_parts, axis=0).T

    attn = jnp.concatenate(
        [orow[pl.ds(h // 2 + 16 * (h % 2), batch, stride=32), :] for h in range(32)], axis=1
    ).astype(BF16)
    cp_wo.wait()
    o_rows = wo.shape[0] // CHUNKS
    half = n_cols // HALVES

    def copy_tp(u):
        return pltpu.make_async_remote_copy(
            src_ref=ypart.at[u], dst_ref=ypeer.at[u], send_sem=tpsend.at[u], recv_sem=tprecv.at[u],
            device_id={"sp": me, "tp": 1 - core},
        )

    for u in range(HALVES):
        y = jnp.zeros((batch, half), F32)
        for c in range(CHUNKS):
            y += jnp.dot(
                attn[:, c * o_rows:(c + 1) * o_rows],
                wo[c * o_rows:(c + 1) * o_rows, u * half:(u + 1) * half],
                preferred_element_type=F32,
            )
        ypart[u] = y
        copy_tp(u).start()
    cp_tp = [copy_tp(u) for u in range(HALVES)]
    for u in range(HALVES):
        cp_tp[u].wait_recv()
        yall[u, cell] = ypart[u] + ypeer[u]
        for a, b in plane_steps:
            pltpu.make_async_remote_copy(
                src_ref=yall.at[u, cell], dst_ref=yall.at[u, cell], send_sem=ysend.at[u], recv_sem=yrecv.at[u],
                device_id={"sp": plane_peer(a, b), "tp": core},
            ).start()

    sum_bytes(gathered.at[pl.ds(0, 16 * (PLANE - 1))], qsend)
    for t in range(3):
        for p in range(len(PARTS)):
            sum_bytes(parts[p].at[t, pl.ds(0, SIDE - 1)], part_send.at[p, t])
    for u in range(HALVES):
        cp_tp[u].wait_send()

    for u in range(HALVES):
        sum_bytes(yall.at[u, pl.ds(0, PLANE - 1)], yrecv.at[u])
        for i in range(PLANE):
            lo = i * n_cols + u * half
            out_ref[:, lo:lo + half] = (hid[:, lo:lo + half].astype(F32) + yall[u, i]).astype(BF16)
    for u in range(HALVES):
        sum_bytes(yall.at[u, pl.ds(0, PLANE - 1)], ysend.at[u])


def store_kernel(y_ref, k_ref, v_ref, out_ref, ko_ref, vo_ref, sems):
    copies = []
    for b in range(k_ref.shape[0]):
        copies.append(pltpu.make_async_copy(k_ref.at[b], ko_ref.at[b], sems.at[2 * b]))
        copies.append(pltpu.make_async_copy(v_ref.at[b], vo_ref.at[b], sems.at[2 * b + 1]))
    copies.append(pltpu.make_async_copy(y_ref, out_ref, sems.at[2 * k_ref.shape[0]]))
    for cp in copies:
        cp.start()
    for cp in copies:
        cp.wait()


def solution(mesh):
    def local_step(hidden, norm_gain, w_query, w_key, w_value, w_out, k_cache, v_cache, positions):
        batch, seq_local, kv_local, head = k_cache.shape
        d_model = hidden.shape[1]
        n_cols = w_out.shape[1] // PLANE
        half = np.arange(head // 2, dtype=np.float32) * np.float32(2.0) / np.float32(head)
        inv = (np.float32(1.0) / np.power(np.float32(ROPE_BASE), half)).astype(np.float32)
        freq = jnp.asarray(np.concatenate([inv, inv])[None, :])
        flat = (batch, seq_local * kv_local, head)
        hbm = pl.BlockSpec(memory_space=pltpu.HBM)
        vmem = pl.BlockSpec(memory_space=pltpu.VMEM)
        dma = pltpu.SemaphoreType.DMA
        y, k_next, v_next = pl.pallas_call(
            attention_kernel,
            out_shape=[
                jax.ShapeDtypeStruct(hidden.shape, BF16),
                jax.ShapeDtypeStruct(flat, BF16),
                jax.ShapeDtypeStruct(flat, BF16),
            ],
            in_specs=[hbm] * 10,
            out_specs=[vmem] * 3,
            scratch_shapes=[
                pltpu.VMEM(hidden.shape, BF16),
                pltpu.VMEM((1, d_model), F32),
                pltpu.VMEM((1, head), F32),
                pltpu.VMEM((d_model, 256), BF16),
                pltpu.VMEM((d_model // SIDE, head), BF16),
                pltpu.VMEM((d_model // SIDE, head), BF16),
                pltpu.VMEM((w_out.shape[0], n_cols), BF16),
                pltpu.VMEM((batch, head, seq_local * kv_local), BF16),
                pltpu.VMEM((PLANE * 16, head), F32),
                pltpu.VMEM((32, head), F32),
                pltpu.VMEM((batch, d_model), F32),
                *[pltpu.VMEM((3, SIDE, d + 8 * stats, 128), F32) for _, d, stats in PARTS],
                pltpu.VMEM((128, 128), F32),
                pltpu.VMEM((128, 128), F32),
                pltpu.VMEM((HALVES, batch, n_cols // HALVES), F32),
                pltpu.VMEM((HALVES, batch, n_cols // HALVES), F32),
                pltpu.VMEM((HALVES, PLANE, batch, n_cols // HALVES), F32),
                pltpu.SMEM((batch,), jnp.int32),
                dma((9,)),
                dma((CHUNKS,)),
                dma((len(PARTS), 3)),
                dma((len(PARTS), 3)),
                dma, dma,
                *[dma((HALVES,))] * 4,
            ],
            compiler_params=pltpu.CompilerParams(
                collective_id=0, has_side_effects=True, vmem_limit_bytes=30 << 20
            ),
            cost_estimate=pl.CostEstimate(flops=20_000_000_000, bytes_accessed=20_000_000, transcendentals=0),
            name="attention_step",
        )(
            *[
                pltpu.with_memory_space_constraint(a, pltpu.HBM)
                for a in (
                    hidden, norm_gain.reshape(1, d_model), freq, positions, w_query, w_key, w_value, w_out,
                    k_cache.reshape(flat), v_cache.reshape(flat),
                )
            ]
        )
        any_space = pl.BlockSpec(memory_space=pl.ANY)
        y, k_next, v_next = pl.pallas_call(
            store_kernel,
            out_shape=[
                jax.ShapeDtypeStruct(hidden.shape, BF16),
                jax.ShapeDtypeStruct(flat, BF16),
                jax.ShapeDtypeStruct(flat, BF16),
            ],
            in_specs=[vmem] * 3,
            out_specs=[any_space] * 3,
            scratch_shapes=[dma((2 * batch + 1,))],
            compiler_params=pltpu.CompilerParams(vmem_limit_bytes=16 << 20),
            cost_estimate=pl.CostEstimate(flops=1_000_000, bytes_accessed=8_000_000, transcendentals=0),
            name="cache_store",
        )(y, k_next, v_next)
        return y, k_next.reshape(k_cache.shape), v_next.reshape(v_cache.shape)

    cache_spec = P("dp", "sp", "tp", None)
    specs_in = (P("dp", None), P(None), P(None, "tp"), P(None, "tp"), P(None, "tp"), P("tp", None), cache_spec, cache_spec, P("dp"))
    specs_out = (P("dp", None), cache_spec, cache_spec)
    return jax.shard_map(local_step, mesh=mesh, in_specs=specs_in, out_specs=specs_out, check_vma=False)
```
